32 devices in a mesh: atom: 16 (over z, y, core), band: 2 (over x).
Axes of the slice: x: 2, y: 2, z: 4, core: 2. Of those that a mesh axis runs over, the one named last changes fastest.
Arguments:
- wave_rows: bfloat16 [256, 65536], P('atom', 'band'), may hold values from -6 to 6
- projectors: bfloat16 [2048, 65536], P('atom', 'band'), may hold values from -0.0234375 to 0.0234375
- dij_table: float32 [16, 8, 8], replicated, may hold values from -6 to 6
- dij_index: int32 [256], P('atom'), may hold values from 0 to 15
- proj_count: int32 [256], P('atom'), may hold values from 1 to 8
Outputs:
- nonlocal_rows: bfloat16 [256, 65536], P('atom', 'band')
The draws below stay inside these ranges and needn't reach their ends.
All inputs are finite; a program needn't handle non-finite values.
Results may differ from the reference program's by a relative error of at most 0.0049.
Values may be sent and summed in bfloat16 or wider, within the bound.
A program may use at most 128 MiB of HBM per device.

```python
import jax
import jax.numpy as jnp
from jax import lax

G = 65536
PROJ = 8
KINDS = 16
ATOMS = 256
BANDS = 256


def touch_ends(entries, rng, smallest, high):
    extent = entries.shape
    index_at = [jax.random.randint(jax.random.fold_in(rng, axis), (), 0, extent[axis]) for axis in range(len(extent))]
    entries = entries.at[tuple(index_at)].set(smallest)
    longest = extent.index(max(extent))
    index_at[longest] = (index_at[longest] + 1) % extent[longest]
    return entries.at[tuple(index_at)].set(high)


def block_levels(own_key, dims, shards, smallest, high):
    loudness, own = 1.0, jax.random.fold_in(own_key, 6)
    for dim, parts in shards:
        heights = jnp.exp(jax.random.uniform(jax.random.fold_in(own, dim), (parts,), jnp.float32, smallest / len(shards), high / len(shards)))
        loudness = loudness * jnp.repeat(heights, dims[dim] // parts).reshape([-1 if axis == dim else 1 for axis in range(len(dims))])
    return loudness


def scatter_about(key, dims, width, limit, pieces=(), held_as=jnp.bfloat16):
    values = jax.random.normal(key, dims, jnp.float32) * width
    if len(pieces) > 0:
        values = block_levels(key, dims, pieces, -0.22, 0.18) * values
    return jnp.clip(values, min=-limit, max=limit).astype(held_as)


def setup_inputs(seed: int = 0) -> dict:
    key_list = jax.random.split(jax.random.key(seed), 6)
    return {
        "wave_rows": scatter_about(key_list[0], (BANDS, G), 1.0, 6.0, ((0, 16), (1, 2))),
        "projectors": scatter_about(key_list[1], (ATOMS * PROJ, G), G ** -0.5, 0.0234375, ((0, 16), (1, 2))),
        "dij_table": scatter_about(key_list[2], (KINDS, PROJ, PROJ), 1.0, 6.0, (), jnp.float32),
        "dij_index": touch_ends(jax.random.randint(key_list[3], (ATOMS,), 0, KINDS), jax.random.fold_in(key_list[3], 1), 0, KINDS - 1).astype(jnp.int32),
        "proj_count": touch_ends(jax.random.randint(key_list[4], (ATOMS,), 1, PROJ + 1), jax.random.fold_in(key_list[4], 1), 1, PROJ).astype(jnp.int32),
    }


def reference(wave_rows, projectors, dij_table, dij_index, proj_count):
    intersections = jnp.dot(wave_rows, projectors.T, preferred_element_type=jnp.float32)
    kind_onehot = (dij_index[:, None] == jnp.arange(KINDS, dtype=jnp.int32)[None, :]).astype(jnp.float32)
    blocks = jnp.dot(kind_onehot, dij_table.reshape(KINDS, PROJ * PROJ), precision=lax.Precision.HIGHEST).reshape(ATOMS, PROJ, PROJ)
    active = (jnp.arange(PROJ, dtype=jnp.int32)[None, :] < proj_count[:, None]).astype(jnp.float32)
    blocks = blocks * active[:, :, None] * active[:, None, :]
    weighted = jnp.einsum("baj,aij->bai", intersections.reshape(BANDS, ATOMS, PROJ), blocks, precision=lax.Precision.HIGHEST)
    weighted = weighted.reshape(BANDS, ATOMS * PROJ).astype(jnp.bfloat16)
    return jnp.dot(weighted, projectors, preferred_element_type=jnp.float32).astype(jnp.bfloat16)
```

```python
import functools

import jax
import jax.numpy as jnp
from jax import lax
from jax.experimental import pallas as pl
from jax.experimental.pallas import tpu as pltpu
from jax.sharding import PartitionSpec as P

MESH = pl.DeviceIdType.MESH
GROUPS = 2
GATHER_SHARE = (0.8125, 0.5)
SCATTER_SHARE = (0.5, 0.8125)


def mix_matrix(table, index, count):
    atoms = index.shape[0]
    kinds, per_atom = table.shape[:2]
    depth = atoms * per_atom
    exact = functools.partial(
        lax.dot_general, precision=lax.Precision.HIGHEST, preferred_element_type=jnp.float32)

    def iota(shape, axis):
        return lax.broadcasted_iota(jnp.int32, shape, axis)

    row, lane = iota((depth, depth), 0), iota((depth, depth), 1)
    spread = (iota((depth, atoms), 0) // per_atom == iota((depth, atoms), 1)).astype(jnp.float32)
    pick = (lax.rem(iota((depth, per_atom), 0), per_atom) == iota((depth, per_atom), 1)).astype(
        jnp.float32)
    plain = (((1,), (0,)), ((), ()))

    def over_rows(value):
        value = jnp.broadcast_to(value.astype(jnp.float32), (atoms, depth))
        return exact(spread, value, plain)

    kind, active = over_rows(index), over_rows(count)
    chosen = jnp.zeros((depth, depth), jnp.float32)
    for k in range(kinds):
        turned = exact(pick, table[k], (((1,), (1,)), ((), ())))
        wide = exact(turned, pick, (((1,), (1,)), ((), ())))
        chosen = jnp.where(jnp.abs(kind - k) < 0.5, wide, chosen)
    inside = lax.rem(row, per_atom).astype(jnp.float32) < active - 0.5
    inside &= lax.rem(lane, per_atom).astype(jnp.float32) < active - 0.5
    inside &= row // per_atom == lane // per_atom
    return jnp.where(inside, chosen, 0.0)


def chunks_of(width, share):
    unit = max(width // 32, 128)
    units = width // unit
    single = min(max(round(share * units), 1), units)
    first = (single + 1) // 2
    cuts = [(0, first, True), (first, single - first, True), (single, units - single, False)]
    return [(start * unit, size * unit, kind) for start, size, kind in cuts if size]


def flows_of(chunks):
    return ([(c, 0) for c, chunk in enumerate(chunks) if chunk[2]]
            + [(c, lane) for c, chunk in enumerate(chunks) if not chunk[2] for lane in range(2)])


def kernel(length, bands, gather_plan, scatter_plan, wave, proj, table, index, count, out, gath,
           full, term, ysend, yrecv, slot, inter, swap, parts, mixes, weights, own_sem, wave_sem,
           proj_sem, mix_sem, az_s, az_r, ay_s, ay_r, rz_s, rz_r, ry_s, ry_r, swap_sem, part_s,
           part_r, wt_sem, out_sem, out_local):
    atom = lax.axis_index("atom")
    band = lax.axis_index("band")
    core = lax.rem(atom, 2)
    other = 1 - core
    y = lax.rem(atom // 2, 2)
    z = atom // 4

    groups, _, _, rows, width = gath.shape
    depth = proj.shape[0]
    both = 2 * depth
    half_rows = length * rows
    unit = max(width // 32, 128)

    def device(lane, place, side):
        return ((place * 2 + lane) * 2 + side, band)

    peer = device(y, z, other)
    across = device(1 - y, z, core)
    toward = (device(y, z + 1, core), device(y, z - 1, core))
    can = (z < length - 1, z > 0)
    edge = (z == 0, z == length - 1)
    partners = [(atom, lax.rem(band + k, bands)) for k in range(1, bands)]

    barrier = pltpu.get_barrier_semaphore()
    for target in [peer, across] + partners:
        pl.semaphore_signal(barrier, inc=1, device_id=target, device_id_type=MESH)
    for d in range(2):
        @pl.when(can[d])
        def _():
            pl.semaphore_signal(barrier, inc=1, device_id=toward[d], device_id_type=MESH)
    pl.semaphore_wait(
        barrier, 2 + len(partners) + can[0].astype(jnp.int32) + can[1].astype(jnp.int32))

    def remote(src, dst, s_sem, r_sem, target):
        return pltpu.make_async_remote_copy(
            src_ref=src, dst_ref=dst, send_sem=s_sem, recv_sem=r_sem,
            device_id=target, device_id_type=MESH)

    def span(side, start, size):
        return pl.ds(pl.multiple_of(side * width + start, 128), size)

    own_copies, peer_out, peer_in = [], [], []
    for sub in range(groups // 2):
        here = pl.ds(sub * rows, rows)
        c = remote(wave.at[here, span(other, 0, width)], gath.at[2 * sub + core, 0, z],
                   wave_sem.at[0, sub], wave_sem.at[1, sub], peer)
        c.start()
        peer_out.append(c)
        c = pltpu.make_async_copy(wave.at[here, span(core, 0, width)],
                                  gath.at[2 * sub + core, 0, z], own_sem.at[sub])
        c.start()
        own_copies.append(c)
        peer_in.append(remote(wave.at[here, span(other, 0, width)],
                              gath.at[2 * sub + other, 0, z],
                              wave_sem.at[0, sub], wave_sem.at[1, sub], peer))

    gather_flows = [flows_of(p) for p in gather_plan]
    scatter_flows = [flows_of(p) for p in scatter_plan]

    def singles(plan):
        return [c for c, chunk in enumerate(plan) if chunk[2]]

    def doubles(plan):
        return [c for c, chunk in enumerate(plan) if not chunk[2]]

    def cols(chunk):
        return pl.ds(chunk[0], chunk[1])

    def a_z(g, f, block, d, own=False):
        c, lane = gather_flows[g][f]
        piece = gath.at[g, lane, block, :, cols(gather_plan[g][c])]
        sent = length if own and d else block
        return remote(piece, piece, az_s.at[g, f, sent], az_r.at[g, f, block], toward[d])

    def a_y(g, c, block):
        where = cols(gather_plan[g][c])
        return remote(gath.at[g, 0, block, :, where], gath.at[g, 1, block, :, where],
                      ay_s.at[g, c, block], ay_r.at[g, c, block], across)

    def own_z(g, d, when, single, lane=0):
        for f, (c, on) in enumerate(gather_flows[g]):
            if gather_plan[g][c][2] == single and on == lane:
                @pl.when(when)
                def _():
                    a_z(g, f, z, d, True).start()

    def own_y(g, single):
        for c in (singles if single else doubles)(gather_plan[g]):
            a_y(g, c, z).start()

    def arrive(g, f, delta):
        c, _ = gather_flows[g][f]
        for d in range(2):
            block = z - delta if d == 0 else z + delta

            @pl.when(block >= 0 if d == 0 else block < length)
            def _():
                copy = a_z(g, f, block, d)
                copy.wait_recv()

                @pl.when(can[d])
                def _():
                    copy.start()
                if gather_plan[g][c][2]:
                    a_y(g, c, block).start()

    def gather_early(g):
        for d in range(2):
            own_z(g, d, can[d] & edge[d], True)

    def gather_open(g, early):
        own_y(g, False)
        for d in range(2):
            own_z(g, d, can[d] & jnp.logical_not(edge[d]) if early else can[d], True)
        own_y(g, True)

    def gather_step(g, delta):
        for f, (c, _) in enumerate(gather_flows[g]):
            if gather_plan[g][c][2]:
                arrive(g, f, delta)
        if delta == 1:
            for d in range(2):
                own_z(g, d, can[d], False)
            for c in doubles(gather_plan[g]):
                a_y(g, c, z).wait_recv()
            for d in range(2):
                own_z(g, d, can[d], False, 1)

    def gather_double(g, delta):
        for f, (c, _) in enumerate(gather_flows[g]):
            if not gather_plan[g][c][2]:
                arrive(g, f, delta)

    def gather_close(g):
        for c in singles(gather_plan[g]):
            for block in range(length):
                a_y(g, c, block).wait_recv()

    kt = min(1024, width)
    keep, give = core, other

    def meet(g):
        def body(t, acc):
            where = pl.ds(pl.multiple_of(t * kt, kt), kt)
            left = gath[g, :, :, :, where].reshape(2 * half_rows, kt)
            return acc + lax.dot_general(left, full[:, where], (((1,), (1,)), ((), ())),
                                         preferred_element_type=jnp.float32)

        total = lax.fori_loop(0, width // kt, body, jnp.zeros((2 * half_rows, both), jnp.float32))
        inter[g] = total.reshape(2, half_rows, both)

    def core_sum(g):
        return remote(inter.at[g, give], swap.at[g], swap_sem.at[0, g], swap_sem.at[1, g], peer)

    def band_sum(g, k):
        return remote(inter.at[g, keep], parts.at[g, k], part_s.at[g, k], part_r.at[g, k],
                      partners[k])

    def share(g, which):
        piece = weights.at[g, which]
        return remote(piece, piece, wt_sem.at[0, g], wt_sem.at[1, g], peer)

    def middle_two(g):
        core_sum(g).wait()
        inter[g, keep] = inter[g, keep] + swap[g]
        for k in range(len(partners)):
            band_sum(g, k).start()

    def middle_three(g):
        value = inter[g, keep]
        for k in range(len(partners)):
            band_sum(g, k).wait()
            value = value + parts[g, k]
        for m in range(2):
            cut = slice(m * depth, (m + 1) * depth)
            weights[g, keep, :, cut] = lax.dot_general(
                value[:, cut], mixes[m], (((1,), (0,)), ((), ())),
                precision=lax.Precision.HIGHEST,
                preferred_element_type=jnp.float32).astype(weights.dtype)
        share(g, keep).start()

    def r_y(g, c, block):
        where = cols(scatter_plan[g][c])
        return remote(ysend.at[g, block, :, where], yrecv.at[g, block, :, where],
                      ry_s.at[g, c, block], ry_r.at[g, c, block], across)

    def r_z(g, f, block, d, last):
        c, lane = scatter_flows[g][f]
        where = cols(scatter_plan[g][c])
        lands = length if last and d else block
        return remote(slot.at[g, lane, block, :, where], slot.at[g, lane, lands, :, where],
                      rz_s.at[g, f, block], rz_r.at[g, f, lands], toward[d])

    def tiles(chunk, body):
        start, size, _ = chunk

        @pl.loop(0, size // unit)
        def _(t):
            body(pl.ds(pl.multiple_of(start + t * unit, unit), unit))

    def apply(g, c):
        chunk = scatter_plan[g][c]

        def body(where):
            new = jnp.dot(weights[g].reshape(2 * half_rows, both), full[:, where],
                          preferred_element_type=jnp.float32)
            if chunk[2]:
                term[g, 0, :, :, where] = new[:half_rows].reshape(length, rows, unit)
                ysend[g, :, :, where] = new[half_rows:].reshape(length, rows, unit).astype(
                    ysend.dtype)
            else:
                term[g, :, :, :, where] = new.reshape(2, length, rows, unit)

        tiles(chunk, body)

    def send_across(g, c):
        for delta in range(length - 1, 0, -1):
            @pl.when(z + delta < length)
            def _():
                r_y(g, c, z + delta).start()

            @pl.when(z - delta >= 0)
            def _():
                r_y(g, c, z - delta).start()
        r_y(g, c, z).start()

    def fold(g, f, delta):
        c, lane = scatter_flows[g][f]
        chunk = scatter_plan[g][c]
        for d in range(2):
            block = z + delta if d == 0 else z - delta

            def run(arrived):
                def body(where):
                    new = term[g, lane, block, :, where]
                    if chunk[2]:
                        new = new + yrecv[g, block, :, where].astype(jnp.float32)
                    if arrived:
                        new = new + slot[g, lane, block, :, where].astype(jnp.float32)
                    slot[g, lane, block, :, where] = new.astype(slot.dtype)

                tiles(chunk, body)

            @pl.when(block < length if d == 0 else block >= 0)
            def _():
                if chunk[2]:
                    r_y(g, c, block).wait_recv()
                if delta < length - 1:
                    @pl.when(can[1 - d])
                    def _():
                        r_z(g, f, block, d, False).wait_recv()
                        run(True)

                    @pl.when(jnp.logical_not(can[1 - d]))
                    def _():
                        run(False)
                else:
                    run(False)
                r_z(g, f, block, d, delta == 1).start()

    def scatter_open(g):
        plan = scatter_plan[g]
        for c in doubles(plan):
            apply(g, c)
        scatter_double(g, length - 1)
        for c in singles(plan):
            apply(g, c)
            send_across(g, c)

    def scatter_double(g, delta):
        for f, (c, _) in enumerate(scatter_flows[g]):
            if not scatter_plan[g][c][2]:
                fold(g, f, delta)

    def scatter_single(g, delta):
        for f, (c, _) in enumerate(scatter_flows[g]):
            if scatter_plan[g][c][2]:
                fold(g, f, delta)

    def result(g, c):
        start, size, _ = scatter_plan[g][c]
        piece = yrecv.at[g, z, :, pl.ds(start, size)]
        here = pl.ds(g // 2 * rows, rows)
        return (pltpu.make_async_copy(piece, out.at[here, span(core, start, size)],
                                      out_local.at[g, c]),
                remote(piece, out.at[here, span(core, start, size)], out_sem.at[0, g, c],
                       out_sem.at[1, g, c], peer),
                remote(piece, out.at[here, span(other, start, size)], out_sem.at[0, g, c],
                       out_sem.at[1, g, c], peer))

    def collect(g, f):
        c, lane = scatter_flows[g][f]
        chunk = scatter_plan[g][c]
        for d in range(2):
            lands = length if d else z

            @pl.when(can[1 - d])
            def _():
                r_z(g, f, z, d, True).wait_recv()

                def body(where):
                    term[g, lane, z, :, where] = (
                        term[g, lane, z, :, where]
                        + slot[g, lane, lands, :, where].astype(jnp.float32))

                tiles(chunk, body)

    def collect_across(g):
        for f, (c, lane) in enumerate(scatter_flows[g]):
            if lane:
                collect(g, f)

                def body(where):
                    ysend[g, z, :, where] = term[g, 1, z, :, where].astype(ysend.dtype)

                tiles(scatter_plan[g][c], body)
                r_y(g, c, z).start()

    def collect_own(g, single):
        for f, (c, lane) in enumerate(scatter_flows[g]):
            if lane == 0 and scatter_plan[g][c][2] == single:
                collect(g, f)
                r_y(g, c, z).wait_recv()

                def body(where):
                    new = term[g, 0, z, :, where] + yrecv[g, z, :, where].astype(jnp.float32)
                    yrecv[g, z, :, where] = new.astype(yrecv.dtype)

                tiles(scatter_plan[g][c], body)
                local, far, _ = result(g, c)

                @pl.when(core == g % 2)
                def _():
                    local.start()

                @pl.when(core != g % 2)
                def _():
                    far.start()

    def entered(sub):
        own_copies[sub].wait()
        peer_in[sub].wait_recv()

    entered(0)
    gather_open(0, False)

    mine = pl.ds(pl.multiple_of(core * depth, depth), depth)
    theirs = pl.ds(pl.multiple_of(other * depth, depth), depth)
    proj_local = pltpu.make_async_copy(proj.at[:, span(core, 0, width)], full.at[mine, :],
                                       own_sem.at[groups // 2])
    proj_local.start()
    proj_out = remote(proj.at[:, span(other, 0, width)], full.at[mine, :], proj_sem.at[0],
                      proj_sem.at[1], peer)
    proj_out.start()
    proj_in = remote(proj.at[:, span(other, 0, width)], full.at[theirs, :], proj_sem.at[0],
                     proj_sem.at[1], peer)
    mixes[core] = mix_matrix(table, index[...], count[...])
    mix_out = remote(mixes.at[core], mixes.at[core], mix_sem.at[0], mix_sem.at[1], peer)
    mix_out.start()
    mix_in = remote(mixes.at[other], mixes.at[other], mix_sem.at[0], mix_sem.at[1], peer)
    for sub in range(1, groups // 2):
        entered(sub)

    gather_step(0, 1)
    gather_early(1)
    for delta in range(2, length):
        gather_step(0, delta)
    for delta in range(1, length):
        gather_double(0, delta)
    gather_open(1, True)
    proj_local.wait()
    proj_in.wait_recv()
    mix_in.wait_recv()
    gather_close(0)
    meet(0)
    core_sum(0).start()

    for g in range(groups):
        more = g + 1 < groups
        middle_two(g)
        if more:
            gather_step(g + 1, 1)
            if g + 2 < groups:
                gather_early(g + 2)
        if g:
            scatter_single(g - 1, 1)
        middle_three(g)
        share(g, give).wait_recv()
        scatter_open(g)
        if g:
            collect_across(g - 1)
            collect_own(g - 1, True)
        for delta in range(length - 2, 0, -1):
            if more:
                gather_step(g + 1, length - delta)
            scatter_double(g, delta)
        if g:
            collect_own(g - 1, False)
        for delta in range(length - 1, 1, -1):
            if more:
                gather_double(g + 1, length - delta)
            scatter_single(g, delta)
        if more:
            gather_double(g + 1, length - 1)
            if g + 2 < groups:
                gather_open(g + 2, True)
            gather_close(g + 1)
            meet(g + 1)
            core_sum(g + 1).start()

    collect_across(groups - 1)
    scatter_single(groups - 1, 1)
    collect_own(groups - 1, False)
    collect_own(groups - 1, True)

    for sub in range(groups // 2):
        peer_out[sub].wait_send()
    proj_out.wait_send()
    mix_out.wait_send()
    for g in range(groups):
        share(g, keep).wait_send()
        for f, (c, lane) in enumerate(gather_flows[g]):
            @pl.loop(0, length)
            def _(block):
                @pl.when((block <= z) & can[0])
                def _():
                    a_z(g, f, block, 0).wait_send()

                @pl.when((block > z) & can[1])
                def _():
                    a_z(g, f, block, 1).wait_send()

            @pl.when(can[1])
            def _():
                a_z(g, f, z, 1, True).wait_send()
        for f in range(len(scatter_flows[g])):
            @pl.loop(0, length)
            def _(block):
                @pl.when(block != z)
                def _():
                    r_z(g, f, block, 0, False).wait_send()
        for c, chunk in enumerate(gather_plan[g]):
            if chunk[2]:
                @pl.loop(0, length)
                def _(block):
                    a_y(g, c, block).wait_send()
            else:
                a_y(g, c, z).wait_send()
        for c, chunk in enumerate(scatter_plan[g]):
            if chunk[2]:
                @pl.loop(0, length)
                def _(block):
                    r_y(g, c, block).wait_send()
            else:
                r_y(g, c, z).wait_send()
            local, far, coming = result(g, c)

            @pl.when(core == g % 2)
            def _():
                local.wait()
                coming.wait_recv()

            @pl.when(core != g % 2)
            def _():
                far.wait_send()


def shards(chips, bands, wave_rows, projectors, dij_table, dij_index, proj_count):
    depth = dij_index.shape[0] * dij_table.shape[1]
    all_rows, columns = wave_rows.shape
    length = chips // 2
    width = columns // 2
    both = 2 * depth
    groups = GROUPS
    rows = 2 * all_rows // groups
    others = max(bands - 1, 1)
    gather_plan = [chunks_of(width, share) for share in GATHER_SHARE]
    scatter_plan = [chunks_of(width, share) for share in SCATTER_SHARE]
    chunks = max(len(p) for p in gather_plan + scatter_plan)
    flows = max(len(flows_of(p)) for p in gather_plan + scatter_plan)
    dma = pltpu.SemaphoreType.DMA
    f32, bf16 = jnp.float32, jnp.bfloat16
    anywhere = pl.BlockSpec(memory_space=pl.ANY)
    return pl.pallas_call(
        functools.partial(kernel, length, bands, gather_plan, scatter_plan),
        out_shape=jax.ShapeDtypeStruct((all_rows, columns), bf16),
        in_specs=[anywhere, anywhere] + [pl.BlockSpec(memory_space=pltpu.VMEM)] * 3,
        out_specs=anywhere,
        scratch_shapes=[
            pltpu.VMEM((groups, 2, length, rows, width), bf16),
            pltpu.VMEM((both, width), bf16),
            pltpu.VMEM((groups, 2, length, rows, width), f32),
            pltpu.VMEM((groups, length, rows, width), bf16),
            pltpu.VMEM((groups, length, rows, width), bf16),
            pltpu.VMEM((groups, 2, length + 1, rows, width), bf16),
            pltpu.VMEM((groups, 2, length * rows, both), f32),
            pltpu.VMEM((groups, length * rows, both), f32),
            pltpu.VMEM((groups, others, length * rows, both), f32),
            pltpu.VMEM((2, depth, depth), f32),
            pltpu.VMEM((groups, 2, length * rows, both), bf16),
            dma((groups // 2 + 1,)), dma((2, groups // 2)), dma((2,)), dma((2,)),
            dma((groups, flows, length + 1)), dma((groups, flows, length)),
            dma((groups, chunks, length)), dma((groups, chunks, length)),
            dma((groups, flows, length)), dma((groups, flows, length + 1)),
            dma((groups, chunks, length)), dma((groups, chunks, length)),
            dma((2, groups)), dma((groups, others)), dma((groups, others)), dma((2, groups)),
            dma((2, groups, chunks)), dma((groups, chunks)),
        ],
        compiler_params=pltpu.CompilerParams(
            collective_id=0, has_side_effects=True, vmem_limit_bytes=60 * 1024 * 1024
        ),
    )(wave_rows, projectors, dij_table, dij_index[:, None], proj_count[:, None])


def solution(mesh):
    in_specs = (P("atom", "band"), P("atom", "band"), P(), P("atom"), P("atom"))
    chips = mesh.shape["atom"] // 2
    bands = mesh.shape["band"]
    return jax.jit(
        jax.shard_map(
            functools.partial(shards, chips, bands),
            mesh=mesh,
            in_specs=in_specs,
            out_specs=P("atom", "band"),
            check_vma=False,
        )
    )
```

```python
import functools

import jax
import jax.numpy as jnp
from jax import lax
from jax.experimental import pallas as pl
from jax.experimental.pallas import tpu as pltpu
from jax.sharding import PartitionSpec as P

MESH = pl.DeviceIdType.MESH
GROUPS = 4
ANY, EDGE, INNER = range(3)
GATHER_SHARE = (0.8125, 0.625, 0.5625, 0.5625)
SCATTER_SHARE = (0.5625, 0.5625, 0.625, 0.8125)
PARTS = (2, 1)


def mix_matrix(table, index, count):
    atoms = index.shape[0]
    kinds, per_atom = table.shape[:2]
    depth = atoms * per_atom
    exact = functools.partial(
        lax.dot_general, precision=lax.Precision.HIGHEST, preferred_element_type=jnp.float32)

    def iota(shape, axis):
        return lax.broadcasted_iota(jnp.int32, shape, axis)

    row, lane = iota((depth, depth), 0), iota((depth, depth), 1)
    spread = (iota((depth, atoms), 0) // per_atom == iota((depth, atoms), 1)).astype(jnp.float32)
    pick = (lax.rem(iota((depth, per_atom), 0), per_atom) == iota((depth, per_atom), 1)).astype(
        jnp.float32)
    plain = (((1,), (0,)), ((), ()))

    def over_rows(value):
        value = jnp.broadcast_to(value.astype(jnp.float32), (atoms, depth))
        return exact(spread, value, plain)

    kind, active = over_rows(index), over_rows(count)
    chosen = jnp.zeros((depth, depth), jnp.float32)
    for k in range(kinds):
        turned = exact(pick, table[k], (((1,), (1,)), ((), ())))
        wide = exact(turned, pick, (((1,), (1,)), ((), ())))
        chosen = jnp.where(jnp.abs(kind - k) < 0.5, wide, chosen)
    inside = lax.rem(row, per_atom).astype(jnp.float32) < active - 0.5
    inside &= lax.rem(lane, per_atom).astype(jnp.float32) < active - 0.5
    inside &= row // per_atom == lane // per_atom
    return jnp.where(inside, chosen, 0.0)


def chunks_of(width, share):
    unit = max(width // 32, 128)
    units = width // unit
    single = min(max(round(share * units), 1), units)
    cuts = []
    for at, size, parts, kind in ((0, single, PARTS[0], True),
                                  (single, units - single, PARTS[1], False)):
        for p in range(parts):
            low, high = size * p // parts, size * (p + 1) // parts
            cuts.append((at + low, high - low, kind))
    return [(start * unit, size * unit, kind) for start, size, kind in cuts if size]


def flows_of(chunks):
    return ([(c, 0) for c, chunk in enumerate(chunks) if chunk[2]]
            + [(c, lane) for c, chunk in enumerate(chunks) if not chunk[2] for lane in range(2)])


SLOTS = [
    ("az", 3, 1, 0, EDGE, [0]),
    ("az", 0, 1, 0, ANY, [1]),
    ("ay", 0, 2, [2]),
    ("az", 0, 1, 1, ANY, [3]),
    ("az", 0, 0, 0, ANY, [4]),
    ("az", 2, 1, 0, EDGE, [5]),
    ("az", 2, 1, 1, EDGE, [6]),
    ("az", 0, 0, 1, ANY, [7]),
    ("ay", 2, 2, [8]),
    ("ay", 0, 1, [9]),
    ("ew", 0, 2, [10]),
    ("az", 0, 2, 0, ANY, [11]),
    ("az", 1, 1, 0, EDGE, [12]),
    ("az", 0, 3, 1, ANY, [13]),
    ("ar", 0, 1, 1, [14, 23, 26]),
    ("ar", 0, 1, 0, [15, 21, 27]),
    ("az", 2, 0, 1, INNER, [16]),
    ("ar", 0, 0, 0, [17, 32, 35]),
    ("az", 0, 2, 1, ANY, [18]),
    ("az", 2, 0, 0, EDGE, [19]),
    ("az", 0, 3, 0, ANY, [20]),
    ("ay", 0, 0, [22]),
    ("ar", 0, 2, 0, [24, 36, 41]),
    ("ar", 0, 0, 1, [25, 29, 37]),
    ("ar", 0, 3, 1, [28, 40, 60]),
    ("az", 1, 0, 1, EDGE, [30]),
    ("az", 1, 0, 0, EDGE, [31]),
    ("ar", 0, 2, 1, [33, 39, 62]),
    ("az", 3, 0, 1, EDGE, [34]),
    ("ew", 2, 2, [38]),
    ("az", 2, 0, 1, EDGE, [42]),
    ("ay", 1, 2, [43]),
    ("ar", 0, 3, 0, [44, 48, 51]),
    ("az", 2, 1, 1, INNER, [45]),
    ("az", 2, 1, 0, INNER, [46]),
    ("az", 2, 0, 0, INNER, [47]),
    ("az", 1, 2, 0, ANY, [49]),
    ("az", 2, 2, 1, ANY, [50]),
    ("ay", 2, 1, [52]),
    ("az", 2, 3, 1, ANY, [53]),
    ("ar", 2, 1, 0, [54, 85, 101]),
    ("az", 3, 0, 0, EDGE, [55]),
    ("az", 2, 2, 0, ANY, [56]),
    ("ar", 2, 0, 1, [57, 79, 97]),
    ("ar", 2, 1, 1, [58, 76, 89]),
    ("az", 1, 1, 1, EDGE, [59]),
    ("close", 0, [61]),
    ("ar", 2, 0, 0, [63, 75, 91]),
    ("ay", 3, 1, [64]),
    ("ay", 3, 2, [65]),
    ("az", 2, 3, 0, ANY, [66]),
    ("meet", 0, [67]),
    ("ay", 2, 0, [68]),
    ("az", 3, 1, 1, EDGE, [69]),
    ("ar", 2, 2, 1, [70, 81, 108]),
    ("ay", 1, 1, [71]),
    ("ar", 2, 3, 1, [72, 82, 120]),
    ("ar", 2, 2, 0, [73, 96, 115]),
    ("m2", 0, [74]),
    ("m3", 0, [77]),
    ("ew", 1, 2, [78]),
    ("ar", 2, 3, 0, [80, 95, 112]),
    ("az", 3, 2, 1, ANY, [83]),
    ("sh", 0, [84]),
    ("az", 1, 0, 1, INNER, [86]),
    ("ap", 0, 2, [87]),
    ("az", 1, 1, 1, INNER, [88]),
    ("fo", 0, 3, 0, [207, 109, 90]),
    ("ew", 3, 2, [92]),
    ("fo", 0, 3, 1, [218, 114, 93]),
    ("ap", 0, 0, [94]),
    ("az", 3, 3, 1, ANY, [98]),
    ("fo", 0, 2, 1, [228, 133, 99]),
    ("ys", 0, 0, [121, 110, 100]),
    ("ap", 0, 1, [102]),
    ("ys", 0, 1, [126, 103, 113]),
    ("fo", 0, 0, 1, [220, 128, 104]),
    ("az", 1, 3, 1, ANY, [105]),
    ("az", 1, 3, 0, ANY, [106]),
    ("az", 3, 2, 0, ANY, [107]),
    ("az", 1, 0, 0, INNER, [111]),
    ("az", 1, 1, 0, INNER, [116]),
    ("fo", 0, 2, 0, [191, 144, 117]),
    ("yo", 0, 0, [118]),
    ("az", 1, 2, 1, ANY, [119]),
    ("close", 2, [122]),
    ("meet", 2, [123]),
    ("fo", 0, 1, 0, [222, 142, 124]),
    ("ar", 1, 0, 1, [125, 150, 173]),
    ("ar", 1, 1, 1, [127, 163, 176]),
    ("az", 3, 1, 1, INNER, [129]),
    ("ar", 1, 0, 0, [130, 136, 154]),
    ("m2", 2, [131]),
    ("ar", 1, 1, 0, [132, 145, 180]),
    ("az", 3, 3, 0, ANY, [134]),
    ("fo", 0, 0, 0, [224, 177, 135]),
    ("ay", 1, 0, [137]),
    ("fo", 0, 1, 1, [225, 146, 138]),
    ("ar", 1, 2, 0, [139, 170, 203]),
    ("m3", 2, [140]),
    ("ar", 1, 3, 0, [141, 172, 206]),
    ("ar", 1, 3, 1, [143, 181, 198]),
    ("sh", 2, [147]),
    ("ap", 2, 2, [148]),
    ("az", 3, 0, 0, INNER, [149]),
    ("ar", 1, 2, 1, [151, 178, 193]),
    ("fo", 2, 2, 1, [204, 165, 152]),
    ("fo", 2, 2, 0, [214, 164, 153]),
    ("fo", 2, 3, 1, [200, 171, 155]),
    ("az", 3, 0, 1, INNER, [156]),
    ("ap", 2, 0, [157]),
    ("ys", 2, 0, [182, 162, 158]),
    ("fo", 2, 3, 0, [226, 167, 159]),
    ("ap", 2, 1, [160]),
    ("ys", 2, 1, [190, 168, 161]),
    ("az", 3, 1, 0, INNER, [166]),
    ("fo", 2, 0, 0, [245, 192, 169]),
    ("fo", 2, 1, 0, [229, 202, 174]),
    ("fo", 2, 0, 1, [217, 195, 175]),
    ("fo", 2, 1, 1, [242, 201, 179]),
    ("ar", 3, 1, 0, [183, 210, 239]),
    ("ar", 3, 0, 0, [184, 209, 234]),
    ("ar", 3, 3, 0, [185, 219, 256]),
    ("yo", 2, 0, [186]),
    ("ar", 3, 2, 1, [187, 215, 243]),
    ("ar", 3, 2, 0, [188, 221, 259]),
    ("ar", 3, 1, 1, [189, 212, 231]),
    ("ar", 3, 0, 1, [194, 213, 236]),
    ("yo", 2, 1, [196]),
    ("ar", 3, 3, 1, [197, 216, 253]),
    ("ay", 3, 0, [199]),
    ("close", 1, [205]),
    ("meet", 1, [208]),
    ("yo", 0, 1, [211]),
    ("m2", 1, [223]),
    ("m3", 1, [227]),
    ("sh", 1, [230]),
    ("ap", 1, 2, [232]),
    ("fo", 1, 3, 0, [263, 246, 233]),
    ("fo", 1, 3, 1, [264, 251, 235]),
    ("ap", 1, 0, [237]),
    ("ys", 1, 0, [247, 250, 238]),
    ("fo", 1, 2, 1, [272, 252, 240]),
    ("fo", 1, 2, 0, [314, 257, 241]),
    ("ap", 1, 1, [244]),
    ("ys", 1, 1, [255, 258, 248]),
    ("yo", 1, 0, [249]),
    ("fo", 1, 0, 1, [283, 271, 254]),
    ("close", 3, [260]),
    ("meet", 3, [261]),
    ("fo", 1, 0, 0, [285, 270, 262]),
    ("fo", 1, 1, 1, [294, 276, 265]),
    ("m2", 3, [266]),
    ("yo", 1, 1, [267]),
    ("fo", 1, 1, 0, [288, 275, 268]),
    ("ca", 2, 3, [269]),
    ("ca", 0, 3, [273]),
    ("m3", 3, [274]),
    ("co", 2, 1, [277]),
    ("sh", 3, [278]),
    ("ap", 3, 1, [279]),
    ("ys", 3, 1, [291, 282, 280]),
    ("ap", 3, 2, [281]),
    ("fo", 3, 2, 1, [327, 296, 284]),
    ("ap", 3, 0, [286]),
    ("fo", 3, 3, 0, [307, 292, 287]),
    ("ys", 3, 0, [301, 290, 289]),
    ("fo", 3, 3, 1, [318, 309, 293]),
    ("fo", 3, 1, 0, [317, 305, 295]),
    ("fo", 3, 2, 0, [324, 312, 297]),
    ("co", 0, 0, [298]),
    ("co", 0, 2, [299]),
    ("fo", 3, 1, 1, [319, 313, 300]),
    ("ca", 1, 3, [302]),
    ("fo", 3, 0, 0, [320, 311, 303]),
    ("fo", 3, 0, 1, [323, 315, 304]),
    ("co", 2, 2, [306]),
    ("co", 0, 1, [308]),
    ("yo", 3, 1, [310]),
    ("co", 2, 0, [316]),
    ("yo", 3, 0, [321]),
    ("co", 1, 0, [322]),
    ("co", 1, 1, [325]),
    ("ca", 3, 3, [326]),
    ("co", 3, 1, [328]),
    ("co", 1, 2, [329]),
    ("co", 3, 0, [330]),
    ("co", 3, 2, [331]),
]


def order_of(length):
    keyed = []
    for name, group, *rest, slots in SLOTS:
        if len(slots) == 1:
            keyed.append((slots[0], (name, group, *rest)))
            continue
        for delta in range(1, length):
            at = (delta - 1) * (len(slots) - 1) / max(length - 2, 1)
            low = min(int(at), len(slots) - 2)
            key = slots[low] + (at - low) * (slots[low + 1] - slots[low])
            keyed.append((key, (name, group, delta, *rest)))
    return [step for _, step in sorted(keyed, key=lambda pair: pair[0])]


def kernel(length, bands, gather_plan, scatter_plan, steps, wave, proj, table, index, count, out,
           gath, full, term, ysend, yrecv, slot, inter, swap, parts, mixes, weights, own_sem, wave_sem,
           proj_sem, mix_sem, az_s, az_r, ay_s, ay_r, rz_s, rz_r, ry_s, ry_r, swap_sem, part_s,
           part_r, wt_sem, out_sem, out_local):
    atom = lax.axis_index("atom")
    band = lax.axis_index("band")
    core = lax.rem(atom, 2)
    other = 1 - core
    y = lax.rem(atom // 2, 2)
    z = atom // 4

    groups, _, _, rows, width = gath.shape
    depth = proj.shape[0]
    both = 2 * depth
    half_rows = length * rows
    unit = max(width // 32, 128)

    def device(lane, place, side):
        return ((place * 2 + lane) * 2 + side, band)

    peer = device(y, z, other)
    across = device(1 - y, z, core)
    toward = (device(y, z + 1, core), device(y, z - 1, core))
    can = (z < length - 1, z > 0)
    edge = (z == 0, z == length - 1)
    partners = [(atom, lax.rem(band + k, bands)) for k in range(1, bands)]

    barrier = pltpu.get_barrier_semaphore()
    for target in [peer, across] + partners:
        pl.semaphore_signal(barrier, inc=1, device_id=target, device_id_type=MESH)
    for d in range(2):
        @pl.when(can[d])
        def _():
            pl.semaphore_signal(barrier, inc=1, device_id=toward[d], device_id_type=MESH)
    pl.semaphore_wait(
        barrier, 2 + len(partners) + can[0].astype(jnp.int32) + can[1].astype(jnp.int32))

    def remote(src, dst, s_sem, r_sem, target):
        return pltpu.make_async_remote_copy(
            src_ref=src, dst_ref=dst, send_sem=s_sem, recv_sem=r_sem,
            device_id=target, device_id_type=MESH)

    def span(side, start, size):
        return pl.ds(pl.multiple_of(side * width + start, 128), size)

    own_copies, peer_out, peer_in = [], [], []
    for sub in range(groups // 2):
        here = pl.ds(sub * rows, rows)
        c = remote(wave.at[here, span(other, 0, width)], gath.at[2 * sub + core, 0, z],
                   wave_sem.at[0, sub], wave_sem.at[1, sub], peer)
        c.start()
        peer_out.append(c)
        c = pltpu.make_async_copy(wave.at[here, span(core, 0, width)],
                                  gath.at[2 * sub + core, 0, z], own_sem.at[sub])
        c.start()
        own_copies.append(c)
        peer_in.append(remote(wave.at[here, span(other, 0, width)],
                              gath.at[2 * sub + other, 0, z],
                              wave_sem.at[0, sub], wave_sem.at[1, sub], peer))

    gather_flows = [flows_of(p) for p in gather_plan]
    scatter_flows = [flows_of(p) for p in scatter_plan]

    def cols(chunk):
        return pl.ds(chunk[0], chunk[1])

    def a_z(g, f, block, d, own=False):
        c, lane = gather_flows[g][f]
        piece = gath.at[g, lane, block, :, cols(gather_plan[g][c])]
        sent = length if own and d else block
        return remote(piece, piece, az_s.at[g, f, sent], az_r.at[g, f, block], toward[d])

    def a_y(g, c, block):
        where = cols(gather_plan[g][c])
        return remote(gath.at[g, 0, block, :, where], gath.at[g, 1, block, :, where],
                      ay_s.at[g, c, block], ay_r.at[g, c, block], across)

    def start_across(g, c):
        a_y(g, c, z).start()

    def start_along(g, f, d, part):
        when = can[d]
        if part == EDGE:
            when = when & edge[d]
        if part == INNER:
            when = when & jnp.logical_not(edge[d])

        @pl.when(when)
        def _():
            a_z(g, f, z, d, True).start()

    def enter(g, c):
        a_y(g, c, z).wait_recv()

    def arrive(g, delta, f, d):
        c, _ = gather_flows[g][f]
        block = z - delta if d == 0 else z + delta

        @pl.when(block >= 0 if d == 0 else block < length)
        def _():
            copy = a_z(g, f, block, d)
            copy.wait_recv()

            @pl.when(can[d])
            def _():
                copy.start()
            if gather_plan[g][c][2]:
                a_y(g, c, block).start()

    def gather_close(g):
        for c, chunk in enumerate(gather_plan[g]):
            if chunk[2]:
                for block in range(length):
                    a_y(g, c, block).wait_recv()

    kt = min(1024, width)
    keep, give = core, other

    def meet(g):
        if g == 0:
            proj_local.wait()
            proj_in.wait_recv()
            mix_in.wait_recv()

        def body(t, acc):
            where = pl.ds(pl.multiple_of(t * kt, kt), kt)
            left = gath[g, :, :, :, where].reshape(2 * half_rows, kt)
            return acc + lax.dot_general(left, full[:, where], (((1,), (1,)), ((), ())),
                                         preferred_element_type=jnp.float32)

        total = lax.fori_loop(0, width // kt, body, jnp.zeros((2 * half_rows, both), jnp.float32))
        inter[g] = total.reshape(2, half_rows, both)
        core_sum(g).start()

    def core_sum(g):
        return remote(inter.at[g, give], swap.at[g], swap_sem.at[0, g], swap_sem.at[1, g], peer)

    def band_sum(g, k):
        return remote(inter.at[g, keep], parts.at[g, k], part_s.at[g, k], part_r.at[g, k],
                      partners[k])

    def share(g, which):
        piece = weights.at[g, which]
        return remote(piece, piece, wt_sem.at[0, g], wt_sem.at[1, g], peer)

    def middle_two(g):
        core_sum(g).wait()
        inter[g, keep] = inter[g, keep] + swap[g]
        for k in range(len(partners)):
            band_sum(g, k).start()

    def middle_three(g):
        value = inter[g, keep]
        for k in range(len(partners)):
            band_sum(g, k).wait()
            value = value + parts[g, k]
        for m in range(2):
            cut = slice(m * depth, (m + 1) * depth)
            weights[g, keep, :, cut] = lax.dot_general(
                value[:, cut], mixes[m], (((1,), (0,)), ((), ())),
                precision=lax.Precision.HIGHEST,
                preferred_element_type=jnp.float32).astype(weights.dtype)
        share(g, keep).start()

    def shared(g):
        share(g, give).wait_recv()

    def r_y(g, c, block):
        where = cols(scatter_plan[g][c])
        return remote(ysend.at[g, block, :, where], yrecv.at[g, block, :, where],
                      ry_s.at[g, c, block], ry_r.at[g, c, block], across)

    def r_z(g, f, block, d, last):
        c, lane = scatter_flows[g][f]
        where = cols(scatter_plan[g][c])
        lands = length if last and d else block
        return remote(slot.at[g, lane, block, :, where], slot.at[g, lane, lands, :, where],
                      rz_s.at[g, f, block], rz_r.at[g, f, lands], toward[d])

    def tiles(chunk, body):
        start, size, _ = chunk

        @pl.loop(0, size // unit)
        def _(t):
            body(pl.ds(pl.multiple_of(start + t * unit, unit), unit))

    def apply(g, c):
        chunk = scatter_plan[g][c]

        def body(where):
            new = jnp.dot(weights[g].reshape(2 * half_rows, both), full[:, where],
                          preferred_element_type=jnp.float32)
            if chunk[2]:
                term[g, 0, :, :, where] = new[:half_rows].reshape(length, rows, unit)
                ysend[g, :, :, where] = new[half_rows:].reshape(length, rows, unit).astype(
                    ysend.dtype)
            else:
                term[g, :, :, :, where] = new.reshape(2, length, rows, unit)

        tiles(chunk, body)

    def send_own_across(g, c):
        r_y(g, c, z).start()

    def send_across(g, delta, c):
        for block in (z + delta, z - delta):
            @pl.when((block >= 0) & (block < length))
            def _():
                r_y(g, c, block).start()

    def fold(g, delta, f, d):
        c, lane = scatter_flows[g][f]
        chunk = scatter_plan[g][c]
        block = z + delta if d == 0 else z - delta

        def run(arrived):
            def body(where):
                new = term[g, lane, block, :, where]
                if chunk[2]:
                    new = new + yrecv[g, block, :, where].astype(jnp.float32)
                if arrived:
                    new = new + slot[g, lane, block, :, where].astype(jnp.float32)
                slot[g, lane, block, :, where] = new.astype(slot.dtype)

            tiles(chunk, body)

        @pl.when(block < length if d == 0 else block >= 0)
        def _():
            if chunk[2]:
                r_y(g, c, block).wait_recv()
            if delta < length - 1:
                @pl.when(can[1 - d])
                def _():
                    r_z(g, f, block, d, False).wait_recv()
                    run(True)

                @pl.when(jnp.logical_not(can[1 - d]))
                def _():
                    run(False)
            else:
                run(False)
            r_z(g, f, block, d, delta == 1).start()

    def result(g, c):
        start, size, _ = scatter_plan[g][c]
        piece = yrecv.at[g, z, :, pl.ds(start, size)]
        here = pl.ds(g // 2 * rows, rows)
        return (pltpu.make_async_copy(piece, out.at[here, span(core, start, size)],
                                      out_local.at[g, c]),
                remote(piece, out.at[here, span(core, start, size)], out_sem.at[0, g, c],
                       out_sem.at[1, g, c], peer),
                remote(piece, out.at[here, span(other, start, size)], out_sem.at[0, g, c],
                       out_sem.at[1, g, c], peer))

    def collect(g, f):
        c, lane = scatter_flows[g][f]
        chunk = scatter_plan[g][c]
        for d in range(2):
            lands = length if d else z

            @pl.when(can[1 - d])
            def _():
                r_z(g, f, z, d, True).wait_recv()

                def body(where):
                    term[g, lane, z, :, where] = (
                        term[g, lane, z, :, where]
                        + slot[g, lane, lands, :, where].astype(jnp.float32))

                tiles(chunk, body)

    def collect_across(g, f):
        c, _ = scatter_flows[g][f]
        collect(g, f)

        def body(where):
            ysend[g, z, :, where] = term[g, 1, z, :, where].astype(ysend.dtype)

        tiles(scatter_plan[g][c], body)
        r_y(g, c, z).start()

    def collect_own(g, f):
        c, _ = scatter_flows[g][f]
        collect(g, f)
        r_y(g, c, z).wait_recv()

        def body(where):
            new = term[g, 0, z, :, where] + yrecv[g, z, :, where].astype(jnp.float32)
            yrecv[g, z, :, where] = new.astype(yrecv.dtype)

        tiles(scatter_plan[g][c], body)
        local, far, _ = result(g, c)

        @pl.when(core == g % 2)
        def _():
            local.start()

        @pl.when(core != g % 2)
        def _():
            far.start()

    def entered(sub):
        own_copies[sub].wait()
        peer_in[sub].wait_recv()

    run = dict(
        ay=start_across, az=start_along, ew=enter, ar=arrive, close=gather_close, meet=meet,
        m2=middle_two, m3=middle_three, sh=shared, ap=apply, ys=send_across,
        yo=send_own_across, fo=fold, ca=collect_across, co=collect_own)
    mine = pl.ds(pl.multiple_of(core * depth, depth), depth)
    theirs = pl.ds(pl.multiple_of(other * depth, depth), depth)
    proj_local = pltpu.make_async_copy(proj.at[:, span(core, 0, width)], full.at[mine, :],
                                       own_sem.at[groups // 2])
    proj_out = remote(proj.at[:, span(other, 0, width)], full.at[mine, :], proj_sem.at[0],
                      proj_sem.at[1], peer)
    proj_in = remote(proj.at[:, span(other, 0, width)], full.at[theirs, :], proj_sem.at[0],
                     proj_sem.at[1], peer)
    mix_out = remote(mixes.at[core], mixes.at[core], mix_sem.at[0], mix_sem.at[1], peer)
    mix_in = remote(mixes.at[other], mixes.at[other], mix_sem.at[0], mix_sem.at[1], peer)

    def prepare():
        proj_local.start()
        proj_out.start()
        mixes[core] = mix_matrix(table, index[...], count[...])
        mix_out.start()

    inside, prepared = set(), False
    for name, g, *rest in steps:
        if name in ("ay", "az"):
            if g // 2 not in inside:
                entered(g // 2)
                inside.add(g // 2)
        elif not prepared:
            prepare()
            prepared = True
        run[name](g, *rest)

    for sub in range(groups // 2):
        peer_out[sub].wait_send()
    proj_out.wait_send()
    mix_out.wait_send()
    for g in range(groups):
        share(g, keep).wait_send()
        for f, (c, lane) in enumerate(gather_flows[g]):
            @pl.loop(0, length)
            def _(block):
                @pl.when((block <= z) & can[0])
                def _():
                    a_z(g, f, block, 0).wait_send()

                @pl.when((block > z) & can[1])
                def _():
                    a_z(g, f, block, 1).wait_send()

            @pl.when(can[1])
            def _():
                a_z(g, f, z, 1, True).wait_send()
        for f in range(len(scatter_flows[g])):
            @pl.loop(0, length)
            def _(block):
                @pl.when(block != z)
                def _():
                    r_z(g, f, block, 0, False).wait_send()
        for c, chunk in enumerate(gather_plan[g]):
            if chunk[2]:
                @pl.loop(0, length)
                def _(block):
                    a_y(g, c, block).wait_send()
            else:
                a_y(g, c, z).wait_send()
        for c, chunk in enumerate(scatter_plan[g]):
            if chunk[2]:
                @pl.loop(0, length)
                def _(block):
                    r_y(g, c, block).wait_send()
            else:
                r_y(g, c, z).wait_send()
            local, far, coming = result(g, c)

            @pl.when(core == g % 2)
            def _():
                local.wait()
                coming.wait_recv()

            @pl.when(core != g % 2)
            def _():
                far.wait_send()


def shards(chips, bands, wave_rows, projectors, dij_table, dij_index, proj_count):
    depth = dij_index.shape[0] * dij_table.shape[1]
    all_rows, columns = wave_rows.shape
    length = chips // 2
    width = columns // 2
    both = 2 * depth
    groups = GROUPS
    rows = 2 * all_rows // groups
    others = max(bands - 1, 1)
    gather_plan = [chunks_of(width, share) for share in GATHER_SHARE]
    scatter_plan = [chunks_of(width, share) for share in SCATTER_SHARE]
    steps = order_of(length)
    chunks = max(len(p) for p in gather_plan + scatter_plan)
    flows = max(len(flows_of(p)) for p in gather_plan + scatter_plan)
    dma = pltpu.SemaphoreType.DMA
    f32, bf16 = jnp.float32, jnp.bfloat16
    anywhere = pl.BlockSpec(memory_space=pl.ANY)
    return pl.pallas_call(
        functools.partial(kernel, length, bands, gather_plan, scatter_plan, steps),
        out_shape=jax.ShapeDtypeStruct((all_rows, columns), bf16),
        in_specs=[anywhere, anywhere] + [pl.BlockSpec(memory_space=pltpu.VMEM)] * 3,
        out_specs=anywhere,
        scratch_shapes=[
            pltpu.VMEM((groups, 2, length, rows, width), bf16),
            pltpu.VMEM((both, width), bf16),
            pltpu.VMEM((groups, 2, length, rows, width), f32),
            pltpu.VMEM((groups, length, rows, width), bf16),
            pltpu.VMEM((groups, length, rows, width), bf16),
            pltpu.VMEM((groups, 2, length + 1, rows, width), bf16),
            pltpu.VMEM((groups, 2, length * rows, both), f32),
            pltpu.VMEM((groups, length * rows, both), f32),
            pltpu.VMEM((groups, others, length * rows, both), f32),
            pltpu.VMEM((2, depth, depth), f32),
            pltpu.VMEM((groups, 2, length * rows, both), bf16),
            dma((groups // 2 + 1,)), dma((2, groups // 2)), dma((2,)), dma((2,)),
            dma((groups, flows, length + 1)), dma((groups, flows, length)),
            dma((groups, chunks, length)), dma((groups, chunks, length)),
            dma((groups, flows, length)), dma((groups, flows, length + 1)),
            dma((groups, chunks, length)), dma((groups, chunks, length)),
            dma((2, groups)), dma((groups, others)), dma((groups, others)), dma((2, groups)),
            dma((2, groups, chunks)), dma((groups, chunks)),
        ],
        compiler_params=pltpu.CompilerParams(
            collective_id=0, has_side_effects=True, vmem_limit_bytes=60 * 1024 * 1024
        ),
    )(wave_rows, projectors, dij_table, dij_index[:, None], proj_count[:, None])


def solution(mesh):
    in_specs = (P("atom", "band"), P("atom", "band"), P(), P("atom"), P("atom"))
    chips = mesh.shape["atom"] // 2
    bands = mesh.shape["band"]
    return jax.jit(
        jax.shard_map(
            functools.partial(shards, chips, bands),
            mesh=mesh,
            in_specs=in_specs,
            out_specs=P("atom", "band"),
            check_vma=False,
        )
    )
```

```python
import functools

import jax
import jax.numpy as jnp
from jax import lax
from jax.experimental import pallas as pl
from jax.experimental.pallas import tpu as pltpu
from jax.sharding import PartitionSpec as P

MESH = pl.DeviceIdType.MESH
GROUPS = 4
GATHER_SHARE = (0.875, 0.625, 0.5625, 0.5)
SCATTER_SHARE = (0.5, 0.5625, 0.625, 0.875)
PARTS = (2, 1)


def mix_matrix(table, index, count):
    per_atom, _, kinds = table.shape
    atoms = index.shape[0]
    depth = atoms * per_atom

    def iota(shape, axis):
        return lax.broadcasted_iota(jnp.int32, shape, axis)

    def of_atom(values, shape):
        atom_of = iota(shape, 0) // per_atom
        spread = jnp.zeros(shape, jnp.int32)
        for a in range(atoms):
            spread = jnp.where(atom_of == a, values[a], spread)
        return spread

    row, lane = iota((depth, depth), 0), iota((depth, depth), 1)
    active = of_atom(count, (depth, depth))
    is_kind = of_atom(index, (depth, kinds)) == iota((depth, kinds), 1)
    chosen = jnp.zeros((depth, depth), jnp.float32)
    for i in range(per_atom):
        rows = jnp.broadcast_to(table[i][None], (atoms, per_atom, kinds)).reshape(depth, kinds)
        picked = jnp.sum(jnp.where(is_kind, rows, 0.0), axis=1, keepdims=True)
        chosen = jnp.where(lax.rem(lane, per_atom) == i, picked, chosen)
    inside = (lax.rem(row, per_atom) < active) & (lax.rem(lane, per_atom) < active)
    inside &= row // per_atom == lane // per_atom
    return jnp.where(inside, chosen, 0.0)


def chunks_of(width, share):
    unit = max(width // 32, 128)
    units = width // unit
    single = min(max(round(share * units), 1), units)
    cuts = []
    for at, size, parts, kind in ((0, single, PARTS[0], True),
                                  (single, units - single, PARTS[1], False)):
        for p in range(parts):
            low, high = size * p // parts, size * (p + 1) // parts
            cuts.append((at + low, high - low, kind))
    return [(start * unit, size * unit, kind) for start, size, kind in cuts if size]


def flows_of(chunks):
    return ([(c, 0) for c, chunk in enumerate(chunks) if chunk[2]]
            + [(c, lane) for c, chunk in enumerate(chunks) if not chunk[2] for lane in range(2)])


SLOTS = [
    ("az", 0, 1, 1, ([0], [9])),
    ("ay", 0, 2, ([1], [12])),
    ("ay", 0, 0, ([2], [38])),
    ("az", 0, 0, 0, ([3], [29])),
    ("az", 0, 0, 1, ([4], [19])),
    ("ay", 3, 2, ([5], [26])),
    ("az", 0, 1, 0, ([6], [5])),
    ("az", 0, 2, 1, ([7], [8])),
    ("az", 2, 0, 0, ([8], [92])),
    ("az", 3, 1, 0, ([11], [153])),
    ("ay", 1, 2, ([12], [15])),
    ("az", 1, 0, 0, ([13], [48])),
    ("ay", 2, 2, ([14], [21])),
    ("az", 1, 0, 1, ([15], [24])),
    ("ar", 0, 1, 1, ([16, 38, 43], [30, 42, 10])),
    ("ar", 0, 0, 0, ([17, 39, 49], [41, 49, 11])),
    ("az", 2, 2, 1, ([18], [136])),
    ("az", 2, 0, 1, ([19], [89])),
    ("ew", 1, 2, ([20], [56])),
    ("az", 3, 1, 1, ([21], [150])),
    ("ew", 0, 2, ([22], [35])),
    ("ay", 0, 1, ([23], [25])),
    ("az", 0, 2, 0, ([24], [34])),
    ("ar", 0, 2, 1, ([25, 60, 81], [51, 67, 68])),
    ("af", 0, 1, 1, ([26, 53, 45], [36, 63, 372])),
    ("ar", 0, 1, 0, ([27, 30, 46], [31, 46, 47])),
    ("az", 0, 3, 1, ([28], [40])),
    ("az", 0, 3, 0, ([29], [39])),
    ("az", 1, 1, 0, ([31], [18])),
    ("az", 1, 1, 1, ([32], [44])),
    ("af", 0, 1, 0, ([33, 37, 47], [50, 54, 229])),
    ("ar", 0, 0, 1, ([52, 34, 54], [33, 57, 84])),
    ("az", 1, 3, 1, ([35], [85])),
    ("af", 0, 0, 1, ([64, 36, 59], [43, 58, 269])),
    ("ew", 3, 2, ([40], [88])),
    ("ar", 0, 3, 0, ([41, 74, 65], [59, 61, 0])),
    ("af", 0, 0, 0, ([56, 42, 58], [45, 53, 223])),
    ("az", 1, 3, 0, ([44], [72])),
    ("az", 2, 2, 0, ([48], [116])),
    ("ar", 1, 1, 0, ([50, 83, 90], [66, 62, 3])),
    ("ar", 1, 0, 1, ([51, 76, 86], [60, 80, 37])),
    ("az", 2, 1, 1, ([55], [105])),
    ("az", 1, 2, 1, ([57], [91])),
    ("az", 3, 2, 1, ([61], [184])),
    ("ar", 1, 0, 0, ([62, 92, 112], [71, 90, 52])),
    ("cl", 0, 1, ([63], [104])),
    ("az", 1, 2, 0, ([66], [75])),
    ("ay", 1, 0, ([67], [108])),
    ("af", 1, 1, 0, ([68, 119, 106], [77, 76, 28])),
    ("ar", 0, 3, 1, ([73, 69, 80], [65, 74, 1])),
    ("mp", 0, 1, ([70], [117])),
    ("az", 3, 3, 1, ([71], [172])),
    ("ar", 0, 2, 0, ([72, 82, 75], [64, 55, 2])),
    ("az", 3, 0, 0, ([77], [125])),
    ("ar", 1, 1, 1, ([78, 95, 101], [70, 82, 13])),
    ("af", 1, 0, 0, ([79, 98, 117], [119, 95, 355])),
    ("az", 3, 2, 0, ([84], [193])),
    ("mp", 0, 2, ([85], [100])),
    ("cl", 0, 0, ([87], [102])),
    ("af", 1, 0, 1, ([94, 88, 96], [81, 110, 366])),
    ("ay", 3, 1, ([89], [123])),
    ("ew", 2, 2, ([91], [87])),
    ("az", 3, 0, 1, ([93], [139])),
    ("mp", 0, 0, ([97], [106])),
    ("ay", 2, 0, ([99], [17])),
    ("az", 2, 1, 0, ([100], [109])),
    ("az", 3, 3, 0, ([102], [192])),
    ("meet", 0, ([103], [128])),
    ("ay", 1, 1, ([104], [73])),
    ("m2", 0, ([105], [138])),
    ("az", 2, 3, 0, ([107], [122])),
    ("ay", 2, 1, ([108], [126])),
    ("m3", 0, ([109], [149])),
    ("az", 2, 3, 1, ([110], [133])),
    ("af", 1, 1, 1, ([111, 114, 113], [83, 96, 239])),
    ("sh", 0, ([115], [157])),
    ("ap", 0, 2, ([116], [164])),
    ("fo", 0, 2, 0, ([118, 130, 144], [254, 218, 382])),
    ("ar", 1, 3, 0, ([128, 120, 154], [86, 113, 101])),
    ("fo", 0, 3, 1, ([140, 121, 131], [257, 173, 376])),
    ("ar", 2, 0, 0, ([122, 133, 189], [99, 134, 4])),
    ("ay", 3, 0, ([123], [219])),
    ("fo", 0, 2, 1, ([126, 160, 124], [268, 231, 368])),
    ("ar", 1, 3, 1, ([143, 125, 158], [97, 124, 127])),
    ("ar", 2, 0, 1, ([127, 145, 191], [112, 132, 14])),
    ("ap", 0, 0, ([129], [159])),
    ("fo", 0, 3, 0, ([146, 172, 132], [258, 220, 166])),
    ("ys", 0, 0, ([134, 138, 148], [187, 174, 188])),
    ("ap", 0, 1, ([136], [171])),
    ("ys", 0, 1, ([193, 137, 161], [246, 189, 190])),
    ("ar", 1, 2, 1, ([152, 139, 153], [93, 120, 7])),
    ("cl", 1, 0, ([141], [142])),
    ("ar", 2, 1, 0, ([142, 183, 185], [118, 144, 16])),
    ("mp", 1, 0, ([147], [143])),
    ("ar", 2, 1, 1, ([164, 149, 180], [115, 135, 131])),
    ("cl", 1, 1, ([150], [130])),
    ("ar", 1, 2, 0, ([151, 159, 156], [98, 107, 94])),
    ("af", 2, 1, 0, ([155, 205, 203], [121, 161, 32])),
    ("mp", 1, 1, ([157], [137])),
    ("mp", 1, 2, ([162], [129])),
    ("yo", 0, 1, ([165], [179])),
    ("fo", 0, 0, 1, ([170, 166, 184], [289, 232, 263])),
    ("af", 2, 0, 1, ([167, 168, 195], [158, 160, 197])),
    ("meet", 1, ([169], [148])),
    ("fo", 0, 1, 0, ([226, 171, 200], [270, 245, 390])),
    ("ar", 2, 2, 0, ([173, 230, 240], [167, 175, 27])),
    ("af", 2, 0, 0, ([175, 174, 190], [156, 141, 20])),
    ("fo", 0, 0, 0, ([194, 176, 182], [303, 272, 394])),
    ("m2", 1, ([177], [152])),
    ("yo", 0, 0, ([178], [177])),
    ("ar", 2, 3, 0, ([179, 227, 225], [147, 163, 78])),
    ("fo", 0, 1, 1, ([288, 181, 187], [283, 255, 337])),
    ("m3", 1, ([186], [168])),
    ("af", 2, 1, 1, ([197, 209, 188], [140, 146, 354])),
    ("sh", 1, ([192], [176])),
    ("ap", 1, 2, ([196], [215])),
    ("ar", 2, 2, 1, ([198, 214, 234], [145, 162, 114])),
    ("fo", 1, 2, 1, ([236, 220, 199], [286, 227, 224])),
    ("fo", 1, 3, 1, ([228, 263, 201], [281, 236, 237])),
    ("fo", 1, 3, 0, ([237, 202, 207], [264, 253, 293])),
    ("ap", 1, 1, ([204], [183])),
    ("ar", 3, 0, 0, ([219, 206, 258], [154, 191, 204])),
    ("fo", 1, 2, 0, ([261, 222, 208], [261, 243, 248])),
    ("ap", 1, 0, ([211], [180])),
    ("ys", 1, 0, ([216, 223, 212], [214, 200, 386])),
    ("ar", 2, 3, 1, ([213, 221, 239], [151, 169, 185])),
    ("ys", 1, 1, ([250, 232, 215], [251, 216, 325])),
    ("ar", 3, 1, 0, ([217, 266, 277], [182, 205, 23])),
    ("cl", 2, 0, ([218], [194])),
    ("mp", 2, 0, ([224], [195])),
    ("cl", 2, 1, ([229], [181])),
    ("mp", 2, 1, ([231], [201])),
    ("yo", 1, 0, ([233], [300])),
    ("af", 3, 0, 0, ([251, 235, 260], [230, 213, 217])),
    ("ar", 3, 1, 1, ([249, 238, 272], [165, 198, 79])),
    ("mp", 2, 2, ([241], [202])),
    ("af", 3, 1, 1, ([282, 242, 280], [225, 222, 349])),
    ("meet", 2, ([243], [210])),
    ("fo", 1, 0, 1, ([244, 256, 257], [301, 284, 359])),
    ("ar", 3, 0, 1, ([245, 246, 268], [170, 199, 266])),
    ("fo", 1, 1, 0, ([281, 310, 247], [311, 282, 379])),
    ("yo", 1, 1, ([248], [252])),
    ("ar", 3, 3, 1, ([252, 314, 312], [209, 228, 69])),
    ("m2", 2, ([253], [226])),
    ("af", 3, 0, 1, ([254, 262, 269], [203, 241, 297])),
    ("fo", 1, 1, 1, ([338, 328, 255], [315, 265, 206])),
    ("fo", 1, 0, 0, ([264, 321, 259], [330, 308, 233])),
    ("ar", 3, 2, 1, ([265, 295, 316], [221, 256, 155])),
    ("m3", 2, ([267], [234])),
    ("af", 3, 1, 0, ([274, 270, 279], [186, 247, 393])),
    ("sh", 2, ([271], [235])),
    ("ap", 2, 2, ([273], [262])),
    ("fo", 2, 2, 0, ([320, 291, 276], [348, 296, 267])),
    ("fo", 2, 2, 1, ([375, 299, 278], [312, 292, 277])),
    ("ap", 2, 0, ([283], [240])),
    ("fo", 2, 3, 0, ([302, 298, 285], [317, 290, 309])),
    ("fo", 2, 3, 1, ([286, 290, 292], [320, 304, 341])),
    ("ar", 3, 2, 0, ([287, 293, 308], [211, 238, 244])),
    ("ys", 2, 0, ([305, 313, 289], [260, 273, 242])),
    ("ap", 2, 1, ([294], [274])),
    ("ar", 3, 3, 0, ([296, 304, 317], [208, 249, 212])),
    ("ys", 2, 1, ([329, 301, 297], [295, 294, 302])),
    ("cl", 3, 0, ([300], [271])),
    ("mp", 3, 0, ([303], [285])),
    ("cl", 3, 1, ([306], [275])),
    ("mp", 3, 1, ([307], [276])),
    ("yo", 2, 0, ([309], [278])),
    ("yo", 2, 1, ([315], [298])),
    ("mp", 3, 2, ([318], [259])),
    ("meet", 3, ([319], [288])),
    ("fo", 2, 1, 1, ([347, 332, 322], [335, 310, 280])),
    ("fo", 2, 0, 1, ([333, 344, 323], [327, 307, 345])),
    ("m2", 3, ([324], [291])),
    ("ca", 0, 3, ([325], [287])),
    ("fo", 2, 1, 0, ([372, 331, 326], [332, 322, 279])),
    ("fo", 2, 0, 0, ([378, 350, 327], [334, 329, 362])),
    ("m3", 3, ([330], [299])),
    ("sh", 3, ([334], [305])),
    ("ap", 3, 1, ([335], [313])),
    ("ys", 3, 1, ([359, 349, 336], [321, 318, 384])),
    ("ap", 3, 2, ([339], [328])),
    ("ap", 3, 0, ([341], [306])),
    ("fo", 3, 3, 1, ([371, 358, 342], [357, 331, 383])),
    ("ys", 3, 0, ([363, 352, 343], [323, 316, 375])),
    ("fo", 3, 2, 1, ([389, 366, 345], [369, 353, 395])),
    ("fo", 3, 3, 0, ([346, 362, 355], [356, 333, 389])),
    ("fo", 3, 2, 0, ([391, 377, 351], [367, 352, 380])),
    ("fo", 3, 1, 1, ([374, 369, 353], [360, 346, 370])),
    ("co", 0, 0, ([354], [347])),
    ("fo", 3, 1, 0, ([381, 364, 356], [358, 339, 338])),
    ("fo", 3, 0, 1, ([383, 370, 357], [363, 350, 378])),
    ("fo", 3, 0, 0, ([382, 365, 360], [361, 343, 344])),
    ("ca", 2, 3, ([361], [336])),
    ("ca", 1, 3, ([367], [326])),
    ("yo", 3, 0, ([368], [365])),
    ("co", 1, 1, ([373], [351])),
    ("co", 2, 0, ([376], [371])),
    ("co", 1, 0, ([379], [381])),
    ("yo", 3, 1, ([380], [342])),
    ("co", 0, 2, ([384], [340])),
    ("ca", 3, 3, ([385], [373])),
    ("co", 0, 1, ([386], [319])),
    ("co", 2, 1, ([387], [364])),
    ("co", 1, 2, ([388], [374])),
    ("co", 2, 2, ([390], [387])),
    ("co", 3, 0, ([392], [388])),
    ("co", 3, 1, ([394], [385])),
    ("co", 3, 2, ([395], [391])),
]


def waits_of(step, length, gather_plan, scatter_plan):
    name, g, *rest = step
    chunks, flows = gather_plan[g], flows_of(gather_plan[g])
    sums, moves = scatter_plan[g], flows_of(scatter_plan[g])
    steps = range(1, length)
    if name == "az" and flows[rest[0]][1]:
        return [("ew", g, flows[rest[0]][0])]
    if name == "ew":
        return [("ay", g, *rest)]
    if name == "ar":
        delta, f, d = rest
        return [("ar", g, delta - 1, f, d) if delta > 1 else ("az", g, f, d)]
    if name == "af":
        return [("ar", g, *rest)]
    if name in ("cl", "mp"):
        c, = rest
        single = chunks[c][2]
        last = "af" if name == "cl" else "ar"
        waits = [(last, g, delta, f, d) for delta in steps for f, (on, _) in enumerate(flows)
                 if on == c for d in range(2)]
        if name == "cl":
            return waits + [("ay", g, c)]
        return waits + [("cl" if single else "ew", g, c)]
    if name == "meet":
        return [("mp", g, c) for c in range(len(chunks))]
    before = dict(m2="meet", m3="m2", sh="m3", ap="sh")
    if name in before:
        return [(before[name], g)]
    if name in ("ys", "yo"):
        return [("ap", g, rest[-1])]
    if name == "fo":
        delta, f, d = rest
        c, _ = moves[f]
        waits = [("ap", g, c)] + ([("ys", g, delta, c)] if sums[c][2] else [])
        return waits + ([("fo", g, delta + 1, f, d)] if delta + 1 < length else [])
    if name in ("ca", "co"):
        f, = rest
        c, lane = moves[f]
        waits = [("ap", g, c), ("fo", g, 1, f, 0), ("fo", g, 1, f, 1)]
        if not lane:
            waits.append(("yo", g, c) if sums[c][2] else ("ca", g, moves.index((c, 1))))
        return waits
    return []


def orders_of(length, gather_plan, scatter_plan):
    tuned = max(len(slots[0]) for *_, slots in SLOTS) == length - 1
    orders = []
    for which in range(2):
        key = {}
        for name, group, *rest, slots in SLOTS:
            slots = slots[which if tuned else 0]
            if name not in ("ar", "af", "ys", "fo"):
                key[name, group, *rest] = slots[0]
                continue
            for delta in range(1, length):
                at = (delta - 1) * (len(slots) - 1) / max(length - 2, 1)
                low = min(int(at), len(slots) - 2)
                key[name, group, delta, *rest] = (
                    slots[low] + (at - low) * (slots[low + 1] - slots[low]))
        if not tuned:
            moved = True
            while moved:
                moved = False
                for step in key:
                    for wait in waits_of(step, length, gather_plan, scatter_plan):
                        if key[step] <= key[wait]:
                            key[step] = key[wait] + 1e-3
                            moved = True
        orders.append(sorted(key, key=key.get))
    return orders


def kernel(length, bands, gather_plan, scatter_plan, steps, wave, proj, table_in, index_in,
           count_in, out, gath, full, term, ysend, yrecv, slot, inter, swap, parts, mixes, weights,
           table, index, count, small_sem, own_sem, wave_sem, proj_sem, mix_sem, az_s, az_r, ay_s,
           ay_r, rz_s, rz_r, ry_s, ry_r, swap_sem, part_s, part_r, wt_sem, out_sem, out_local):
    atom = lax.axis_index("atom")
    band = lax.axis_index("band")
    core = lax.rem(atom, 2)
    other = 1 - core
    y = lax.rem(atom // 2, 2)
    z = atom // 4

    groups, _, _, rows, width = gath.shape
    depth = proj.shape[0]
    both = 2 * depth
    half_rows = length * rows
    unit = max(width // 32, 128)

    def device(lane, place, side):
        return ((place * 2 + lane) * 2 + side, band)

    peer = device(y, z, other)
    across = device(1 - y, z, core)
    toward = (device(y, z + 1, core), device(y, z - 1, core))
    can = (z < length - 1, z > 0)
    edge = (z == 0, z == length - 1)
    partners = [(atom, lax.rem(band + k, bands)) for k in range(1, bands)]

    def span(side, start, size):
        return pl.ds(pl.multiple_of(side * width + start, 128), size)

    own_copies = []
    for sub in range(groups // 2):
        c = pltpu.make_async_copy(wave.at[pl.ds(sub * rows, rows), span(core, 0, width)],
                                  gath.at[2 * sub + core, 0, z], own_sem.at[sub])
        c.start()
        own_copies.append(c)
    small = [pltpu.make_async_copy(src, dst, small_sem.at[i]) for i, (src, dst) in enumerate(
        ((table_in, table), (index_in, index), (count_in, count)))]
    for copy in small:
        copy.start()

    barrier = pltpu.get_barrier_semaphore()
    for target in [peer, across] + partners:
        pl.semaphore_signal(barrier, inc=1, device_id=target, device_id_type=MESH)
    for d in range(2):
        @pl.when(can[d])
        def _():
            pl.semaphore_signal(barrier, inc=1, device_id=toward[d], device_id_type=MESH)
    pl.semaphore_wait(
        barrier, 2 + len(partners) + can[0].astype(jnp.int32) + can[1].astype(jnp.int32))

    def remote(src, dst, s_sem, r_sem, target):
        return pltpu.make_async_remote_copy(
            src_ref=src, dst_ref=dst, send_sem=s_sem, recv_sem=r_sem,
            device_id=target, device_id_type=MESH)

    own_out = []
    for sub in range(groups // 2):
        c = remote(wave.at[pl.ds(sub * rows, rows), span(other, 0, width)],
                   gath.at[2 * sub + core, 0, z], wave_sem.at[0, sub], wave_sem.at[1, sub], peer)
        c.start()
        own_out.append(c)

    def entered(g):
        sub = g // 2

        @pl.when(core == g % 2)
        def _():
            own_copies[sub].wait()

        @pl.when(core != g % 2)
        def _():
            remote(wave.at[pl.ds(sub * rows, rows), span(other, 0, width)], gath.at[g, 0, z],
                   wave_sem.at[0, sub], wave_sem.at[1, sub], peer).wait_recv()

    gather_flows = [flows_of(p) for p in gather_plan]
    scatter_flows = [flows_of(p) for p in scatter_plan]

    def cols(chunk):
        return pl.ds(chunk[0], chunk[1])

    def a_z(g, f, block, d, own=False):
        c, lane = gather_flows[g][f]
        piece = gath.at[g, lane, block, :, cols(gather_plan[g][c])]
        sent = length if own and d else block
        return remote(piece, piece, az_s.at[g, f, sent], az_r.at[g, f, block], toward[d])

    def a_y(g, c, block):
        where = cols(gather_plan[g][c])
        return remote(gath.at[g, 0, block, :, where], gath.at[g, 1, block, :, where],
                      ay_s.at[g, c, block], ay_r.at[g, c, block], across)

    def start_across(g, c):
        a_y(g, c, z).start()

    def start_along(g, f, d):
        @pl.when(can[d])
        def _():
            a_z(g, f, z, d, True).start()

    def enter(g, c):
        a_y(g, c, z).wait_recv()

    def arrive(g, delta, f, d):
        block = z - delta if d == 0 else z + delta

        @pl.when(block >= 0 if d == 0 else block < length)
        def _():
            copy = a_z(g, f, block, d)
            copy.wait_recv()

            @pl.when(can[d])
            def _():
                copy.start()

    def arrived_across(g, delta, f, d):
        c, _ = gather_flows[g][f]
        block = z - delta if d == 0 else z + delta

        @pl.when(block >= 0 if d == 0 else block < length)
        def _():
            a_y(g, c, block).start()

    def gather_close(g, c):
        for block in range(length):
            a_y(g, c, block).wait_recv()

    keep, give = core, other
    met = set()

    def meet(g, c):
        start, size, _ = gather_plan[g][c]
        kt = next(unit * n for n in (2, 1) if size % (unit * n) == 0)

        def body(t, acc):
            where = pl.ds(pl.multiple_of(start + t * kt, unit), kt)
            left = gath[g, :, :, :, where].reshape(2 * half_rows, kt)
            return acc + lax.dot_general(left, full[:, where], (((1,), (1,)), ((), ())),
                                         preferred_element_type=jnp.float32)

        if g in met:
            total = inter[g].reshape(2 * half_rows, both)
        else:
            total = jnp.zeros((2 * half_rows, both), jnp.float32)
        met.add(g)
        total = lax.fori_loop(0, size // kt, body, total)
        inter[g] = total.reshape(2, half_rows, both)

    def met_all(g):
        core_sum(g).start()

    def core_sum(g):
        return remote(inter.at[g, give], swap.at[g], swap_sem.at[0, g], swap_sem.at[1, g], peer)

    def band_sum(g, k):
        return remote(inter.at[g, keep], parts.at[g, k], part_s.at[g, k], part_r.at[g, k],
                      partners[k])

    def share(g, which):
        piece = weights.at[g, which]
        return remote(piece, piece, wt_sem.at[0, g], wt_sem.at[1, g], peer)

    def middle_two(g):
        core_sum(g).wait()
        inter[g, keep] = inter[g, keep] + swap[g]
        for k in range(len(partners)):
            band_sum(g, k).start()

    def middle_three(g):
        value = inter[g, keep]
        for k in range(len(partners)):
            band_sum(g, k).wait()
            value = value + parts[g, k]
        for m in range(2):
            cut = slice(m * depth, (m + 1) * depth)
            weights[g, keep, :, cut] = lax.dot_general(
                value[:, cut], mixes[m], (((1,), (0,)), ((), ())),
                precision=lax.Precision.HIGHEST,
                preferred_element_type=jnp.float32).astype(weights.dtype)
        share(g, keep).start()

    def shared(g):
        share(g, give).wait_recv()

    def r_y(g, c, block):
        where = cols(scatter_plan[g][c])
        return remote(ysend.at[g, block, :, where], yrecv.at[g, block, :, where],
                      ry_s.at[g, c, block], ry_r.at[g, c, block], across)

    def r_z(g, f, block, d, last):
        c, lane = scatter_flows[g][f]
        where = cols(scatter_plan[g][c])
        lands = length if last and d else block
        return remote(slot.at[g, lane, block, :, where], slot.at[g, lane, lands, :, where],
                      rz_s.at[g, f, block], rz_r.at[g, f, lands], toward[d])

    def tiles(chunk, body):
        start, size, _ = chunk

        @pl.loop(0, size // unit)
        def _(t):
            body(pl.ds(pl.multiple_of(start + t * unit, unit), unit))

    def apply(g, c):
        chunk = scatter_plan[g][c]

        def body(where):
            new = jnp.dot(weights[g].reshape(2 * half_rows, both), full[:, where],
                          preferred_element_type=jnp.float32)
            if chunk[2]:
                term[g, 0, :, :, where] = new[:half_rows].reshape(length, rows, unit)
                ysend[g, :, :, where] = new[half_rows:].reshape(length, rows, unit).astype(
                    ysend.dtype)
            else:
                term[g, :, :, :, where] = new.reshape(2, length, rows, unit)

        tiles(chunk, body)

    def send_own_across(g, c):
        r_y(g, c, z).start()

    def send_across(g, delta, c):
        for block in (z + delta, z - delta):
            @pl.when((block >= 0) & (block < length))
            def _():
                r_y(g, c, block).start()

    def fold(g, delta, f, d):
        c, lane = scatter_flows[g][f]
        chunk = scatter_plan[g][c]
        block = z + delta if d == 0 else z - delta

        def run(arrived):
            def body(where):
                new = term[g, lane, block, :, where]
                if chunk[2]:
                    new = new + yrecv[g, block, :, where].astype(jnp.float32)
                if arrived:
                    new = new + slot[g, lane, block, :, where].astype(jnp.float32)
                slot[g, lane, block, :, where] = new.astype(slot.dtype)

            tiles(chunk, body)

        @pl.when(block < length if d == 0 else block >= 0)
        def _():
            if chunk[2]:
                r_y(g, c, block).wait_recv()
            if delta < length - 1:
                @pl.when(can[1 - d])
                def _():
                    r_z(g, f, block, d, False).wait_recv()
                    run(True)

                @pl.when(jnp.logical_not(can[1 - d]))
                def _():
                    run(False)
            else:
                run(False)
            r_z(g, f, block, d, delta == 1).start()

    def result(g, c):
        start, size, _ = scatter_plan[g][c]
        piece = yrecv.at[g, z, :, pl.ds(start, size)]
        here = pl.ds(g // 2 * rows, rows)
        return (pltpu.make_async_copy(piece, out.at[here, span(core, start, size)],
                                      out_local.at[g, c]),
                remote(piece, out.at[here, span(core, start, size)], out_sem.at[0, g, c],
                       out_sem.at[1, g, c], peer),
                remote(piece, out.at[here, span(other, start, size)], out_sem.at[0, g, c],
                       out_sem.at[1, g, c], peer))

    def collect(g, f):
        c, lane = scatter_flows[g][f]
        chunk = scatter_plan[g][c]
        for d in range(2):
            lands = length if d else z

            @pl.when(can[1 - d])
            def _():
                r_z(g, f, z, d, True).wait_recv()

                def body(where):
                    term[g, lane, z, :, where] = (
                        term[g, lane, z, :, where]
                        + slot[g, lane, lands, :, where].astype(jnp.float32))

                tiles(chunk, body)

    def collect_across(g, f):
        c, _ = scatter_flows[g][f]
        collect(g, f)

        def body(where):
            ysend[g, z, :, where] = term[g, 1, z, :, where].astype(ysend.dtype)

        tiles(scatter_plan[g][c], body)
        r_y(g, c, z).start()

    def collect_own(g, f):
        c, _ = scatter_flows[g][f]
        collect(g, f)
        r_y(g, c, z).wait_recv()

        def body(where):
            new = term[g, 0, z, :, where] + yrecv[g, z, :, where].astype(jnp.float32)
            yrecv[g, z, :, where] = new.astype(yrecv.dtype)

        tiles(scatter_plan[g][c], body)
        local, far, _ = result(g, c)

        @pl.when(core == g % 2)
        def _():
            local.start()

        @pl.when(core != g % 2)
        def _():
            far.start()

    run = dict(
        ay=start_across, az=start_along, ew=enter, ar=arrive, af=arrived_across, cl=gather_close,
        mp=meet, meet=met_all, m2=middle_two, m3=middle_three, sh=shared, ap=apply,
        ys=send_across, yo=send_own_across, fo=fold, ca=collect_across, co=collect_own)
    mine = pl.ds(pl.multiple_of(core * depth, depth), depth)
    theirs = pl.ds(pl.multiple_of(other * depth, depth), depth)
    proj_local = pltpu.make_async_copy(proj.at[:, span(core, 0, width)], full.at[mine, :],
                                       own_sem.at[groups // 2])
    proj_out = remote(proj.at[:, span(other, 0, width)], full.at[mine, :], proj_sem.at[0],
                      proj_sem.at[1], peer)
    proj_in = remote(proj.at[:, span(other, 0, width)], full.at[theirs, :], proj_sem.at[0],
                     proj_sem.at[1], peer)
    mix_out = remote(mixes.at[core], mixes.at[core], mix_sem.at[0], mix_sem.at[1], peer)
    mix_in = remote(mixes.at[other], mixes.at[other], mix_sem.at[0], mix_sem.at[1], peer)

    def prepare():
        proj_local.start()
        proj_out.start()
        for copy in small:
            copy.wait()
        mixes[core] = mix_matrix(table, index, count)
        mix_out.start()

    def play(steps):
        met.clear()
        prepared = ready = False
        inside = set()
        for name, *rest in steps:
            if name in ("ay", "az") and rest[0] not in inside:
                entered(rest[0])
                inside.add(rest[0])
            if not prepared and name not in ("ay", "az"):
                prepare()
                prepared = True
            if not ready and name == "mp":
                proj_local.wait()
                proj_in.wait_recv()
                mix_in.wait_recv()
                ready = True
            run[name](*rest)

    at_end = edge[0] | edge[1]

    @pl.when(at_end)
    def _():
        play(steps[0])

    @pl.when(jnp.logical_not(at_end))
    def _():
        play(steps[1])

    for c in own_out:
        c.wait_send()
    proj_out.wait_send()
    mix_out.wait_send()
    for g in range(groups):
        share(g, keep).wait_send()
        for f, (c, lane) in enumerate(gather_flows[g]):
            @pl.loop(0, length)
            def _(block):
                @pl.when((block <= z) & can[0])
                def _():
                    a_z(g, f, block, 0).wait_send()

                @pl.when((block > z) & can[1])
                def _():
                    a_z(g, f, block, 1).wait_send()

            @pl.when(can[1])
            def _():
                a_z(g, f, z, 1, True).wait_send()
        for f in range(len(scatter_flows[g])):
            @pl.loop(0, length)
            def _(block):
                @pl.when(block != z)
                def _():
                    r_z(g, f, block, 0, False).wait_send()
        for c, chunk in enumerate(gather_plan[g]):
            if chunk[2]:
                @pl.loop(0, length)
                def _(block):
                    a_y(g, c, block).wait_send()
            else:
                a_y(g, c, z).wait_send()
        for c, chunk in enumerate(scatter_plan[g]):
            if chunk[2]:
                @pl.loop(0, length)
                def _(block):
                    r_y(g, c, block).wait_send()
            else:
                r_y(g, c, z).wait_send()
            local, far, coming = result(g, c)

            @pl.when(core == g % 2)
            def _():
                local.wait()
                coming.wait_recv()

            @pl.when(core != g % 2)
            def _():
                far.wait_send()


def shards(chips, bands, wave_rows, projectors, dij_table, dij_index, proj_count):
    depth = dij_index.shape[0] * dij_table.shape[1]
    all_rows, columns = wave_rows.shape
    length = chips // 2
    width = columns // 2
    both = 2 * depth
    groups = GROUPS
    rows = 2 * all_rows // groups
    others = max(bands - 1, 1)
    gather_plan = [chunks_of(width, share) for share in GATHER_SHARE]
    scatter_plan = [chunks_of(width, share) for share in SCATTER_SHARE]
    steps = orders_of(length, gather_plan, scatter_plan)
    chunks = max(len(p) for p in gather_plan + scatter_plan)
    flows = max(len(flows_of(p)) for p in gather_plan + scatter_plan)
    dma = pltpu.SemaphoreType.DMA
    f32, bf16 = jnp.float32, jnp.bfloat16
    anywhere = pl.BlockSpec(memory_space=pl.ANY)
    return pl.pallas_call(
        functools.partial(kernel, length, bands, gather_plan, scatter_plan, steps),
        out_shape=jax.ShapeDtypeStruct((all_rows, columns), bf16),
        in_specs=[anywhere] * 5,
        out_specs=anywhere,
        scratch_shapes=[
            pltpu.VMEM((groups, 2, length, rows, width), bf16),
            pltpu.VMEM((both, width), bf16),
            pltpu.VMEM((groups, 2, length, rows, width), f32),
            pltpu.VMEM((groups, length, rows, width), bf16),
            pltpu.VMEM((groups, length, rows, width), bf16),
            pltpu.VMEM((groups, 2, length + 1, rows, width), bf16),
            pltpu.VMEM((groups, 2, length * rows, both), f32),
            pltpu.VMEM((groups, length * rows, both), f32),
            pltpu.VMEM((groups, others, length * rows, both), f32),
            pltpu.VMEM((2, depth, depth), f32),
            pltpu.VMEM((groups, 2, length * rows, both), bf16),
            pltpu.VMEM(dij_table.shape[1:] + dij_table.shape[:1], f32),
            pltpu.SMEM(dij_index.shape, jnp.int32), pltpu.SMEM(proj_count.shape, jnp.int32),
            dma((3,)), dma((groups // 2 + 1,)), dma((2, groups // 2)), dma((2,)), dma((2,)),
            dma((groups, flows, length + 1)), dma((groups, flows, length)),
            dma((groups, chunks, length)), dma((groups, chunks, length)),
            dma((groups, flows, length)), dma((groups, flows, length + 1)),
            dma((groups, chunks, length)), dma((groups, chunks, length)),
            dma((2, groups)), dma((groups, others)), dma((groups, others)), dma((2, groups)),
            dma((2, groups, chunks)), dma((groups, chunks)),
        ],
        compiler_params=pltpu.CompilerParams(
            collective_id=0, has_side_effects=True, vmem_limit_bytes=60 * 1024 * 1024
        ),
    )(wave_rows, projectors, jnp.transpose(dij_table, (1, 2, 0)), dij_index, proj_count)


def solution(mesh):
    in_specs = (P("atom", "band"), P("atom", "band"), P(), P("atom"), P("atom"))
    chips = mesh.shape["atom"] // 2
    bands = mesh.shape["band"]
    return jax.jit(
        jax.shard_map(
            functools.partial(shards, chips, bands),
            mesh=mesh,
            in_specs=in_specs,
            out_specs=P("atom", "band"),
            check_vma=False,
        )
    )
```

```python
import functools

import jax
import jax.numpy as jnp
from jax import lax
from jax.experimental import pallas as pl
from jax.experimental.pallas import tpu as pltpu
from jax.sharding import PartitionSpec as P

MESH = pl.DeviceIdType.MESH
GROUPS = 4
GATHER_SHARE = (0.84375, 0.59375, 0.53125, 0.5)
SCATTER_SHARE = (0.5, 0.53125, 0.59375, 0.84375)
PARTS = (2, 1)


def mix_matrix(table, index, count):
    per_atom, _, kinds = table.shape
    atoms = index.shape[0]
    depth = atoms * per_atom

    def iota(shape, axis):
        return lax.broadcasted_iota(jnp.int32, shape, axis)

    def of_atom(values, shape):
        atom_of = iota(shape, 0) // per_atom
        spread = jnp.zeros(shape, jnp.int32)
        for a in range(atoms):
            spread = jnp.where(atom_of == a, values[a], spread)
        return spread

    row, lane = iota((depth, depth), 0), iota((depth, depth), 1)
    active = of_atom(count, (depth, depth))
    is_kind = of_atom(index, (depth, kinds)) == iota((depth, kinds), 1)
    chosen = jnp.zeros((depth, depth), jnp.float32)
    for i in range(per_atom):
        rows = jnp.broadcast_to(table[i][None], (atoms, per_atom, kinds)).reshape(depth, kinds)
        picked = jnp.sum(jnp.where(is_kind, rows, 0.0), axis=1, keepdims=True)
        chosen = jnp.where(lax.rem(lane, per_atom) == i, picked, chosen)
    inside = (lax.rem(row, per_atom) < active) & (lax.rem(lane, per_atom) < active)
    inside &= row // per_atom == lane // per_atom
    return jnp.where(inside, chosen, 0.0)


def chunks_of(width, share):
    unit = max(width // 32, 128)
    units = width // unit
    single = min(max(round(share * units), 1), units)
    cuts = []
    for at, size, parts, kind in ((0, single, PARTS[0], True),
                                  (single, units - single, PARTS[1], False)):
        for p in range(parts):
            low, high = size * p // parts, size * (p + 1) // parts
            cuts.append((at + low, high - low, kind))
    return [(start * unit, size * unit, kind) for start, size, kind in cuts if size]


def flows_of(chunks):
    return ([(c, 0) for c, chunk in enumerate(chunks) if chunk[2]]
            + [(c, lane) for c, chunk in enumerate(chunks) if not chunk[2] for lane in range(2)])


SLOTS = [
    ("ay", 0, 2, ([0], [13])),
    ("ay", 2, 2, ([1], [22])),
    ("az", 0, 0, 0, ([2], [0])),
    ("az", 0, 1, 1, ([3], [8])),
    ("az", 0, 1, 0, ([4], [14])),
    ("az", 3, 1, 0, ([5], [69])),
    ("az", 0, 0, 1, ([6], [15])),
    ("az", 0, 2, 0, ([7], [21])),
    ("ay", 1, 2, ([8], [73])),
    ("ar", 0, 0, 0, ([9, 53, 51], [28, 51, 4])),
    ("ew", 0, 2, ([10], [25])),
    ("ar", 0, 1, 1, ([11, 21, 38], [20, 33, 32])),
    ("az", 3, 1, 1, ([12], [148])),
    ("az", 2, 0, 0, ([13], [19])),
    ("ay", 0, 0, ([14], [12])),
    ("az", 1, 2, 0, ([15], [135])),
    ("af", 0, 1, 1, ([16, 23, 50], [23, 40, 392])),
    ("ar", 0, 1, 0, ([17, 31, 47], [24, 37, 54])),
    ("az", 0, 2, 1, ([18], [16])),
    ("az", 0, 3, 1, ([19], [27])),
    ("az", 2, 0, 1, ([20], [30])),
    ("az", 2, 1, 1, ([22], [50])),
    ("af", 0, 0, 0, ([24, 57, 52], [56, 70, 162])),
    ("ew", 2, 2, ([25], [65])),
    ("ar", 0, 2, 1, ([26, 64, 76], [41, 55, 34])),
    ("az", 0, 3, 0, ([27], [35])),
    ("az", 2, 1, 0, ([28], [57])),
    ("ay", 0, 1, ([29], [11])),
    ("ar", 0, 0, 1, ([30, 36, 59], [26, 46, 60])),
    ("az", 2, 2, 0, ([32], [88])),
    ("az", 3, 2, 0, ([33], [204])),
    ("af", 0, 0, 1, ([34, 58, 63], [59, 47, 268])),
    ("az", 1, 1, 0, ([35], [110])),
    ("af", 0, 1, 0, ([44, 37, 48], [31, 48, 97])),
    ("az", 2, 3, 1, ([39], [76])),
    ("ar", 2, 0, 0, ([40, 74, 99], [53, 75, 17])),
    ("az", 2, 2, 1, ([42], [64])),
    ("az", 1, 2, 1, ([43], [137])),
    ("az", 3, 2, 1, ([45], [200])),
    ("az", 2, 3, 0, ([46], [82])),
    ("ar", 0, 3, 0, ([49, 69, 79], [52, 67, 36])),
    ("az", 1, 0, 0, ([54], [79])),
    ("ar", 0, 3, 1, ([55, 60, 81], [49, 58, 39])),
    ("az", 1, 1, 1, ([61], [86])),
    ("ar", 0, 2, 0, ([62, 78, 75], [44, 62, 9])),
    ("az", 1, 0, 1, ([65], [107])),
    ("ay", 3, 2, ([66], [145])),
    ("ay", 3, 0, ([67], [198])),
    ("ew", 1, 2, ([68], [115])),
    ("ay", 1, 1, ([70], [85])),
    ("cl", 0, 1, ([71], [71])),
    ("az", 3, 0, 1, ([72], [122])),
    ("mp", 0, 1, ([73], [80])),
    ("af", 2, 0, 0, ([80, 77, 104], [113, 100, 245])),
    ("mp", 0, 2, ([82], [68])),
    ("ar", 2, 1, 1, ([83, 100, 116], [72, 84, 116])),
    ("cl", 0, 0, ([85], [92])),
    ("mp", 0, 0, ([86], [95])),
    ("meet", 0, ([87], [99])),
    ("az", 1, 3, 1, ([88], [141])),
    ("ar", 2, 1, 0, ([93, 89, 113], [77, 81, 114])),
    ("az", 3, 0, 0, ([90], [181])),
    ("ar", 2, 0, 1, ([91, 108, 110], [61, 74, 5])),
    ("af", 2, 1, 0, ([109, 92, 117], [96, 109, 236])),
    ("af", 2, 0, 1, ([94, 114, 115], [78, 111, 118])),
    ("m2", 0, ([95], [102])),
    ("ay", 2, 0, ([96], [112])),
    ("ew", 3, 2, ([97], [175])),
    ("ar", 3, 1, 0, ([98, 276, 259], [184, 193, 254])),
    ("af", 3, 1, 0, ([102, 288, 261], [232, 233, 266])),
    ("az", 3, 3, 0, ([103], [202])),
    ("ay", 1, 0, ([105], [94])),
    ("az", 3, 3, 1, ([106], [196])),
    ("ay", 2, 1, ([107], [106])),
    ("m3", 0, ([111], [123])),
    ("af", 2, 1, 1, ([112, 121, 118], [108, 89, 253])),
    ("az", 1, 3, 0, ([119], [127])),
    ("ar", 2, 3, 1, ([120, 135, 157], [98, 119, 18])),
    ("sh", 0, ([122], [133])),
    ("ap", 0, 2, ([123], [159])),
    ("fo", 0, 3, 1, ([141, 131, 124], [261, 173, 389])),
    ("fo", 0, 3, 0, ([178, 128, 125], [267, 171, 311])),
    ("ap", 0, 0, ([126], [165])),
    ("ar", 2, 2, 1, ([154, 127, 159], [91, 117, 93])),
    ("fo", 0, 2, 0, ([145, 129, 140], [282, 186, 301])),
    ("fo", 0, 2, 1, ([151, 155, 130], [281, 176, 328])),
    ("ys", 0, 0, ([146, 132, 137], [183, 195, 279])),
    ("ap", 0, 1, ([133], [144])),
    ("ar", 2, 3, 0, ([148, 134, 156], [101, 121, 63])),
    ("ar", 2, 2, 0, ([136, 158, 160], [103, 126, 43])),
    ("ar", 1, 0, 0, ([174, 138, 202], [104, 154, 7])),
    ("ar", 1, 1, 1, ([139, 170, 179], [120, 131, 1])),
    ("ys", 0, 1, ([152, 149, 142], [192, 155, 376])),
    ("cl", 2, 0, ([143], [147])),
    ("mp", 2, 0, ([144], [149])),
    ("cl", 2, 1, ([147], [134])),
    ("mp", 2, 1, ([150], [138])),
    ("ar", 1, 0, 1, ([153, 184, 193], [124, 140, 132])),
    ("mp", 2, 2, ([161], [130])),
    ("meet", 2, ([162], [150])),
    ("af", 1, 0, 0, ([182, 163, 203], [125, 161, 388])),
    ("fo", 0, 0, 1, ([186, 164, 176], [299, 246, 260])),
    ("fo", 0, 0, 0, ([165, 199, 204], [325, 300, 345])),
    ("yo", 0, 0, ([166], [213])),
    ("fo", 0, 1, 0, ([173, 181, 167], [296, 211, 168])),
    ("ar", 1, 1, 0, ([168, 192, 194], [142, 153, 6])),
    ("ay", 3, 1, ([169], [197])),
    ("fo", 0, 1, 1, ([188, 171, 196], [332, 275, 384])),
    ("m2", 2, ([172], [163])),
    ("ar", 1, 2, 0, ([175, 226, 231], [158, 177, 166])),
    ("af", 1, 1, 1, ([177, 191, 197], [156, 170, 391])),
    ("af", 1, 0, 1, ([180, 187, 207], [136, 143, 265])),
    ("ar", 3, 0, 1, ([183, 249, 281], [179, 215, 3])),
    ("af", 1, 1, 0, ([185, 195, 200], [146, 167, 128])),
    ("m3", 2, ([190], [182])),
    ("ar", 1, 3, 0, ([198, 221, 240], [157, 180, 129])),
    ("sh", 2, ([205], [191])),
    ("ap", 2, 2, ([206], [223])),
    ("fo", 2, 3, 0, ([254, 237, 208], [264, 238, 252])),
    ("af", 3, 0, 1, ([209, 277, 283], [207, 256, 194])),
    ("fo", 2, 3, 1, ([215, 230, 210], [257, 231, 368])),
    ("ap", 2, 0, ([212], [205])),
    ("ys", 2, 0, ([220, 214, 213], [228, 219, 214])),
    ("fo", 2, 2, 1, ([243, 244, 216], [272, 227, 284])),
    ("ap", 2, 1, ([217], [208])),
    ("fo", 2, 2, 0, ([225, 218, 222], [274, 234, 338])),
    ("ar", 1, 3, 1, ([224, 219, 234], [151, 169, 105])),
    ("cl", 1, 1, ([223], [188])),
    ("ar", 1, 2, 1, ([235, 227, 239], [152, 172, 38])),
    ("mp", 1, 1, ([228], [199])),
    ("cl", 1, 0, ([229], [201])),
    ("mp", 1, 0, ([232], [203])),
    ("fo", 2, 0, 1, ([267, 245, 233], [331, 304, 393])),
    ("ys", 2, 1, ([251, 238, 236], [237, 226, 255])),
    ("mp", 1, 2, ([241], [185])),
    ("meet", 1, ([242], [206])),
    ("fo", 2, 0, 0, ([256, 246, 262], [285, 271, 243])),
    ("fo", 2, 1, 0, ([279, 264, 247], [318, 259, 247])),
    ("ar", 3, 1, 1, ([269, 271, 248], [174, 190, 10])),
    ("m2", 1, ([253], [212])),
    ("fo", 2, 1, 1, ([287, 265, 257], [298, 277, 316])),
    ("yo", 2, 1, ([258], [287])),
    ("yo", 2, 0, ([260], [216])),
    ("ar", 3, 0, 0, ([266, 263, 275], [187, 209, 248])),
    ("yo", 0, 1, ([268], [242])),
    ("af", 3, 0, 0, ([270, 278, 282], [229, 210, 288])),
    ("ar", 3, 3, 1, ([272, 302, 310], [221, 230, 160])),
    ("ar", 3, 2, 0, ([273, 309, 318], [224, 249, 66])),
    ("m3", 1, ([274], [225])),
    ("ar", 3, 3, 0, ([280, 293, 311], [220, 239, 139])),
    ("ar", 3, 2, 1, ([284, 308, 317], [222, 250, 218])),
    ("af", 3, 1, 1, ([291, 286, 285], [189, 217, 90])),
    ("sh", 1, ([289], [235])),
    ("ap", 1, 2, ([290], [241])),
    ("fo", 1, 2, 0, ([316, 336, 292], [329, 303, 262])),
    ("fo", 1, 2, 1, ([324, 298, 294], [306, 286, 290])),
    ("fo", 1, 3, 1, ([301, 321, 295], [315, 293, 276])),
    ("ap", 1, 0, ([296], [244])),
    ("ys", 1, 0, ([323, 322, 297], [263, 307, 258])),
    ("fo", 1, 3, 0, ([327, 300, 299], [310, 295, 390])),
    ("ap", 1, 1, ([303], [240])),
    ("ys", 1, 1, ([314, 304, 306], [292, 270, 382])),
    ("cl", 3, 0, ([305], [280])),
    ("mp", 3, 0, ([307], [283])),
    ("cl", 3, 1, ([312], [273])),
    ("mp", 3, 1, ([313], [289])),
    ("fo", 1, 0, 0, ([342, 338, 315], [342, 322, 363])),
    ("mp", 3, 2, ([319], [269])),
    ("meet", 3, ([320], [291])),
    ("fo", 1, 1, 0, ([334, 341, 326], [335, 308, 327])),
    ("yo", 1, 0, ([328], [319])),
    ("yo", 1, 1, ([329], [309])),
    ("m2", 3, ([330], [297])),
    ("fo", 1, 0, 1, ([387, 333, 331], [340, 323, 251])),
    ("ca", 0, 3, ([332], [302])),
    ("ca", 2, 3, ([335], [278])),
    ("m3", 3, ([337], [305])),
    ("fo", 1, 1, 1, ([340, 343, 339], [344, 330, 294])),
    ("sh", 3, ([344], [312])),
    ("ap", 3, 0, ([345], [313])),
    ("ys", 3, 0, ([362, 359, 346], [320, 314, 372])),
    ("ap", 3, 2, ([347], [317])),
    ("fo", 3, 2, 1, ([356, 355, 348], [348, 337, 395])),
    ("fo", 3, 3, 1, ([360, 371, 349], [359, 339, 366])),
    ("fo", 3, 3, 0, ([381, 350, 358], [358, 347, 326])),
    ("ap", 3, 1, ([351], [333])),
    ("ys", 3, 1, ([369, 361, 352], [341, 336, 387])),
    ("fo", 3, 2, 0, ([383, 354, 353], [365, 349, 334])),
    ("fo", 3, 0, 1, ([379, 374, 357], [362, 352, 381])),
    ("fo", 3, 0, 0, ([382, 372, 363], [361, 351, 377])),
    ("fo", 3, 1, 0, ([386, 378, 364], [369, 355, 385])),
    ("co", 0, 1, ([366], [375])),
    ("co", 2, 1, ([367], [367])),
    ("fo", 3, 1, 1, ([390, 376, 368], [370, 356, 350])),
    ("ca", 1, 3, ([370], [343])),
    ("yo", 3, 0, ([373], [321])),
    ("co", 2, 2, ([375], [346])),
    ("yo", 3, 1, ([377], [364])),
    ("co", 1, 0, ([380], [378])),
    ("co", 0, 0, ([384], [357])),
    ("co", 0, 2, ([385], [353])),
    ("co", 1, 1, ([388], [360])),
    ("co", 2, 0, ([389], [354])),
    ("ca", 3, 3, ([391], [371])),
    ("co", 3, 0, ([392], [379])),
    ("co", 1, 2, ([393], [373])),
    ("co", 3, 1, ([394], [383])),
    ("co", 3, 2, ([395], [380])),
]


def waits_of(step, length, gather_plan, scatter_plan):
    name, g, *rest = step
    chunks, flows = gather_plan[g], flows_of(gather_plan[g])
    sums, moves = scatter_plan[g], flows_of(scatter_plan[g])
    steps = range(1, length)
    if name == "az" and flows[rest[0]][1]:
        return [("ew", g, flows[rest[0]][0])]
    if name == "ew":
        return [("ay", g, *rest)]
    if name == "ar":
        delta, f, d = rest
        return [("ar", g, delta - 1, f, d) if delta > 1 else ("az", g, f, d)]
    if name == "af":
        return [("ar", g, *rest)]
    if name in ("cl", "mp"):
        c, = rest
        single = chunks[c][2]
        last = "af" if name == "cl" else "ar"
        waits = [(last, g, delta, f, d) for delta in steps for f, (on, _) in enumerate(flows)
                 if on == c for d in range(2)]
        if name == "cl":
            return waits + [("ay", g, c)]
        return waits + [("cl" if single else "ew", g, c)]
    if name == "meet":
        return [("mp", g, c) for c in range(len(chunks))]
    before = dict(m2="meet", m3="m2", sh="m3", ap="sh")
    if name in before:
        return [(before[name], g)]
    if name in ("ys", "yo"):
        return [("ap", g, rest[-1])]
    if name == "fo":
        delta, f, d = rest
        c, _ = moves[f]
        waits = [("ap", g, c)] + ([("ys", g, delta, c)] if sums[c][2] else [])
        return waits + ([("fo", g, delta + 1, f, d)] if delta + 1 < length else [])
    if name in ("ca", "co"):
        f, = rest
        c, lane = moves[f]
        waits = [("ap", g, c), ("fo", g, 1, f, 0), ("fo", g, 1, f, 1)]
        if not lane:
            waits.append(("yo", g, c) if sums[c][2] else ("ca", g, moves.index((c, 1))))
        return waits
    return []


def orders_of(length, gather_plan, scatter_plan):
    tuned = max(len(slots[0]) for *_, slots in SLOTS) == length - 1
    orders = []
    for which in range(2):
        key = {}
        for name, group, *rest, slots in SLOTS:
            slots = slots[which if tuned else 0]
            if name not in ("ar", "af", "ys", "fo"):
                key[name, group, *rest] = slots[0]
                continue
            for delta in range(1, length):
                at = (delta - 1) * (len(slots) - 1) / max(length - 2, 1)
                low = min(int(at), len(slots) - 2)
                key[name, group, delta, *rest] = (
                    slots[low] + (at - low) * (slots[low + 1] - slots[low]))
        if not tuned:
            moved = True
            while moved:
                moved = False
                for step in key:
                    for wait in waits_of(step, length, gather_plan, scatter_plan):
                        if key[step] <= key[wait]:
                            key[step] = key[wait] + 1e-3
                            moved = True
        orders.append(sorted(key, key=key.get))
    return orders


def kernel(length, bands, gather_plan, scatter_plan, steps, wave, proj, table_in, index_in,
           count_in, out, gath, full, term, ysend, yrecv, slot, inter, swap, parts, mixes, weights,
           table, index, count, small_sem, own_sem, wave_sem, proj_sem, mix_sem, az_s, az_r, ay_s,
           ay_r, rz_s, rz_r, ry_s, ry_r, swap_sem, part_s, part_r, wt_sem, out_sem, out_local):
    atom = lax.axis_index("atom")
    band = lax.axis_index("band")
    core = lax.rem(atom, 2)
    other = 1 - core
    y = lax.rem(atom // 2, 2)
    z = atom // 4

    groups, _, _, rows, width = gath.shape
    depth = proj.shape[0]
    both = 2 * depth
    half_rows = length * rows
    unit = max(width // 32, 128)

    def device(lane, place, side):
        return ((place * 2 + lane) * 2 + side, band)

    peer = device(y, z, other)
    across = device(1 - y, z, core)
    toward = (device(y, z + 1, core), device(y, z - 1, core))
    can = (z < length - 1, z > 0)
    at_end = (z == 0) | (z == length - 1)
    partners = [(atom, lax.rem(band + k, bands)) for k in range(1, bands)]

    def span(side, start, size):
        return pl.ds(pl.multiple_of(side * width + start, 128), size)

    own_copies = []
    for sub in range(groups // 2):
        c = pltpu.make_async_copy(wave.at[pl.ds(sub * rows, rows), span(core, 0, width)],
                                  gath.at[2 * sub + core, 0, z], own_sem.at[sub])
        c.start()
        own_copies.append(c)
    small = [pltpu.make_async_copy(src, dst, small_sem.at[i]) for i, (src, dst) in enumerate(
        ((table_in, table), (index_in, index), (count_in, count)))]
    for copy in small:
        copy.start()

    barrier = pltpu.get_barrier_semaphore()
    for target in [peer, across] + partners:
        pl.semaphore_signal(barrier, inc=1, device_id=target, device_id_type=MESH)
    for d in range(2):
        @pl.when(can[d])
        def _():
            pl.semaphore_signal(barrier, inc=1, device_id=toward[d], device_id_type=MESH)
    pl.semaphore_wait(
        barrier, 2 + len(partners) + can[0].astype(jnp.int32) + can[1].astype(jnp.int32))

    def remote(src, dst, s_sem, r_sem, target):
        return pltpu.make_async_remote_copy(
            src_ref=src, dst_ref=dst, send_sem=s_sem, recv_sem=r_sem,
            device_id=target, device_id_type=MESH)

    own_out = []
    for sub in range(groups // 2):
        c = remote(wave.at[pl.ds(sub * rows, rows), span(other, 0, width)],
                   gath.at[2 * sub + core, 0, z], wave_sem.at[0, sub], wave_sem.at[1, sub], peer)
        c.start()
        own_out.append(c)

    def entered(g):
        sub = g // 2

        @pl.when(core == g % 2)
        def _():
            own_copies[sub].wait()

        @pl.when(core != g % 2)
        def _():
            remote(wave.at[pl.ds(sub * rows, rows), span(other, 0, width)], gath.at[g, 0, z],
                   wave_sem.at[0, sub], wave_sem.at[1, sub], peer).wait_recv()

    gather_flows = [flows_of(p) for p in gather_plan]
    scatter_flows = [flows_of(p) for p in scatter_plan]

    def cols(chunk):
        return pl.ds(chunk[0], chunk[1])

    def a_z(g, f, block, d):
        c, lane = gather_flows[g][f]
        piece = gath.at[g, lane, block, :, cols(gather_plan[g][c])]
        return remote(piece, piece, az_s.at[g, f], az_r.at[g, f, block], toward[d])

    def a_y(g, c, block):
        where = cols(gather_plan[g][c])
        return remote(gath.at[g, 0, block, :, where], gath.at[g, 1, block, :, where],
                      ay_s.at[g, c], ay_r.at[g, c], across)

    def start_across(g, c):
        a_y(g, c, z).start()

    def start_along(g, f, d):
        @pl.when(can[d])
        def _():
            a_z(g, f, z, d).start()

    def enter(g, c):
        a_y(g, c, z).wait_recv()

    def arrive(g, delta, f, d):
        block = z - delta if d == 0 else z + delta

        @pl.when(block >= 0 if d == 0 else block < length)
        def _():
            copy = a_z(g, f, block, d)
            copy.wait_recv()

            @pl.when(can[d])
            def _():
                copy.start()

    def arrived_across(g, delta, f, d):
        c, _ = gather_flows[g][f]
        block = z - delta if d == 0 else z + delta

        @pl.when(block >= 0 if d == 0 else block < length)
        def _():
            a_y(g, c, block).start()

    def gather_close(g, c):
        piece = gath.at[g, 1, :, :, cols(gather_plan[g][c])]
        remote(piece, piece, ay_s.at[g, c], ay_r.at[g, c], across).wait_recv()

    def widest(size):
        return next(unit * n for n in (8, 7, 5, 4, 3, 2, 1) if size % (unit * n) == 0)

    keep, give = core, other
    met = set()

    def meet(g, c):
        start, size, _ = gather_plan[g][c]
        kt = widest(size)

        def body(t, acc):
            where = pl.ds(pl.multiple_of(start + t * kt, unit), kt)
            left = gath[g, :, :, :, where].reshape(2 * half_rows, kt)
            return acc + lax.dot_general(left, full[:, where], (((1,), (1,)), ((), ())),
                                         preferred_element_type=jnp.float32)

        if g in met:
            total = inter[g].reshape(2 * half_rows, both)
        else:
            total = jnp.zeros((2 * half_rows, both), jnp.float32)
        met.add(g)
        total = lax.fori_loop(0, size // kt, body, total)
        inter[g] = total.reshape(2, half_rows, both)

    def met_all(g):
        core_sum(g).start()

    def core_sum(g):
        return remote(inter.at[g, give], swap.at[g], swap_sem.at[0, g], swap_sem.at[1, g], peer)

    def band_sum(g, k):
        return remote(inter.at[g, keep], parts.at[g, k], part_s.at[g, k], part_r.at[g, k],
                      partners[k])

    def share(g, which):
        piece = weights.at[g, which]
        return remote(piece, piece, wt_sem.at[0, g], wt_sem.at[1, g], peer)

    def middle_two(g):
        core_sum(g).wait()
        inter[g, keep] = inter[g, keep] + swap[g]
        for k in range(len(partners)):
            band_sum(g, k).start()

    def middle_three(g):
        value = inter[g, keep]
        for k in range(len(partners)):
            band_sum(g, k).wait()
            value = value + parts[g, k]
        for m in range(2):
            cut = slice(m * depth, (m + 1) * depth)
            weights[g, keep, :, cut] = lax.dot_general(
                value[:, cut], mixes[m], (((1,), (0,)), ((), ())),
                precision=lax.Precision.HIGHEST,
                preferred_element_type=jnp.float32).astype(weights.dtype)
        share(g, keep).start()

    def shared(g):
        share(g, give).wait_recv()

    def r_y(g, c, block):
        where = cols(scatter_plan[g][c])
        return remote(ysend.at[g, block, :, where], yrecv.at[g, block, :, where],
                      ry_s.at[g, c], ry_r.at[g, c, block], across)

    def r_z(g, f, block, d, last):
        c, lane = scatter_flows[g][f]
        where = cols(scatter_plan[g][c])
        lands = length if last and d else block
        return remote(slot.at[g, lane, block, :, where], slot.at[g, lane, lands, :, where],
                      rz_s.at[g, f], rz_r.at[g, f, lands], toward[d])

    def tiles(chunk, body):
        start, size, _ = chunk
        wide = widest(size)

        @pl.loop(0, size // wide)
        def _(t):
            body(pl.ds(pl.multiple_of(start + t * wide, unit), wide))

    def apply(g, c):
        chunk = scatter_plan[g][c]

        def body(where):
            new = jnp.dot(weights[g].reshape(2 * half_rows, both), full[:, where],
                          preferred_element_type=jnp.float32)
            if chunk[2]:
                term[g, 0, :, :, where] = new[:half_rows].reshape(length, rows, -1)
                ysend[g, :, :, where] = new[half_rows:].reshape(length, rows, -1).astype(
                    ysend.dtype)
            else:
                term[g, :, :, :, where] = new.reshape(2, length, rows, -1)

        tiles(chunk, body)

    def send_own_across(g, c):
        r_y(g, c, z).start()

    def send_across(g, delta, c):
        for block in (z + delta, z - delta):
            @pl.when((block >= 0) & (block < length))
            def _():
                r_y(g, c, block).start()

    def fold(g, delta, f, d):
        c, lane = scatter_flows[g][f]
        chunk = scatter_plan[g][c]
        block = z + delta if d == 0 else z - delta

        def run(arrived):
            def body(where):
                new = term[g, lane, block, :, where]
                if chunk[2]:
                    new = new + yrecv[g, block, :, where].astype(jnp.float32)
                if arrived:
                    new = new + slot[g, lane, block, :, where].astype(jnp.float32)
                slot[g, lane, block, :, where] = new.astype(slot.dtype)

            tiles(chunk, body)

        @pl.when(block < length if d == 0 else block >= 0)
        def _():
            if chunk[2]:
                r_y(g, c, block).wait_recv()
            if delta < length - 1:
                @pl.when(can[1 - d])
                def _():
                    r_z(g, f, block, d, False).wait_recv()
                    run(True)

                @pl.when(jnp.logical_not(can[1 - d]))
                def _():
                    run(False)
            else:
                run(False)
            r_z(g, f, block, d, delta == 1).start()

    def result(g, c):
        start, size, _ = scatter_plan[g][c]
        piece = yrecv.at[g, z, :, pl.ds(start, size)]
        here = pl.ds(g // 2 * rows, rows)
        return (pltpu.make_async_copy(piece, out.at[here, span(core, start, size)],
                                      out_local.at[g, c]),
                remote(piece, out.at[here, span(core, start, size)], out_sem.at[0, g, c],
                       out_sem.at[1, g, c], peer),
                remote(piece, out.at[here, span(other, start, size)], out_sem.at[0, g, c],
                       out_sem.at[1, g, c], peer))

    def collect(g, f):
        c, lane = scatter_flows[g][f]
        chunk = scatter_plan[g][c]
        for d in range(2):
            lands = length if d else z

            @pl.when(can[1 - d])
            def _():
                r_z(g, f, z, d, True).wait_recv()

                def body(where):
                    term[g, lane, z, :, where] = (
                        term[g, lane, z, :, where]
                        + slot[g, lane, lands, :, where].astype(jnp.float32))

                tiles(chunk, body)

    def collect_across(g, f):
        c, _ = scatter_flows[g][f]
        collect(g, f)

        def body(where):
            ysend[g, z, :, where] = term[g, 1, z, :, where].astype(ysend.dtype)

        tiles(scatter_plan[g][c], body)
        r_y(g, c, z).start()

    def collect_own(g, f):
        c, _ = scatter_flows[g][f]
        collect(g, f)
        r_y(g, c, z).wait_recv()

        def body(where):
            new = term[g, 0, z, :, where] + yrecv[g, z, :, where].astype(jnp.float32)
            yrecv[g, z, :, where] = new.astype(yrecv.dtype)

        tiles(scatter_plan[g][c], body)
        local, far, _ = result(g, c)

        @pl.when(core == g % 2)
        def _():
            local.start()

        @pl.when(core != g % 2)
        def _():
            far.start()

    run = dict(
        ay=start_across, az=start_along, ew=enter, ar=arrive, af=arrived_across, cl=gather_close,
        mp=meet, meet=met_all, m2=middle_two, m3=middle_three, sh=shared, ap=apply,
        ys=send_across, yo=send_own_across, fo=fold, ca=collect_across, co=collect_own)
    mine = pl.ds(pl.multiple_of(core * depth, depth), depth)
    theirs = pl.ds(pl.multiple_of(other * depth, depth), depth)
    proj_local = pltpu.make_async_copy(proj.at[:, span(core, 0, width)], full.at[mine, :],
                                       own_sem.at[groups // 2])
    proj_out = remote(proj.at[:, span(other, 0, width)], full.at[mine, :], proj_sem.at[0],
                      proj_sem.at[1], peer)
    proj_in = remote(proj.at[:, span(other, 0, width)], full.at[theirs, :], proj_sem.at[0],
                     proj_sem.at[1], peer)
    mix_out = remote(mixes.at[core], mixes.at[core], mix_sem.at[0], mix_sem.at[1], peer)
    mix_in = remote(mixes.at[other], mixes.at[other], mix_sem.at[0], mix_sem.at[1], peer)

    def prepare():
        proj_local.start()
        proj_out.start()
        for copy in small:
            copy.wait()
        mixes[core] = mix_matrix(table, index, count)
        mix_out.start()

    def sent(piece, sem):
        remote(piece, piece, sem, sem, peer).wait_send()

    def gather_sent():
        for g in range(groups):
            for c, chunk in enumerate(gather_plan[g]):
                blocks = slice(None) if chunk[2] else pl.ds(z, 1)
                sent(gath.at[g, 0, blocks, :, cols(chunk)], ay_s.at[g, c])
            for f, (c, _) in enumerate(gather_flows[g]):
                where = cols(gather_plan[g][c])

                @pl.when(at_end)
                def _():
                    sent(slot.at[g, 0, pl.ds(0, 1), :, where], az_s.at[g, f])

                @pl.when(jnp.logical_not(at_end))
                def _():
                    sent(slot.at[g, 0, :, :, where], az_s.at[g, f])

    def scatter_sent(which):
        for g in which:
            for c, chunk in enumerate(scatter_plan[g]):
                blocks = slice(None) if chunk[2] else pl.ds(z, 1)
                sent(ysend.at[g, blocks, :, cols(chunk)], ry_s.at[g, c])
            for f, (c, _) in enumerate(scatter_flows[g]):
                sent(slot.at[g, 0, pl.ds(0, length - 1), :, cols(scatter_plan[g][c])],
                     rz_s.at[g, f])

    def play(steps):
        met.clear()
        prepared = ready = False
        inside = set()
        last = steps.index(next(s for s in steps if s[:2] == ("co", groups - 1)))
        for at, (name, *rest) in enumerate(steps):
            if at == last:
                gather_sent()
            if at == len(steps) - 1:
                scatter_sent(range(groups - 1))
            if name in ("ay", "az") and rest[0] not in inside:
                entered(rest[0])
                inside.add(rest[0])
            if not prepared and name not in ("ay", "az"):
                prepare()
                prepared = True
            if not ready and name == "mp":
                proj_local.wait()
                proj_in.wait_recv()
                mix_in.wait_recv()
                ready = True
            run[name](*rest)

    @pl.when(at_end)
    def _():
        play(steps[0])

    @pl.when(jnp.logical_not(at_end))
    def _():
        play(steps[1])

    scatter_sent([groups - 1])
    for c in own_out:
        c.wait_send()
    proj_out.wait_send()
    mix_out.wait_send()
    for g in range(groups):
        share(g, keep).wait_send()
        for c in range(len(scatter_plan[g])):
            local, far, coming = result(g, c)

            @pl.when(core == g % 2)
            def _():
                local.wait()
                coming.wait_recv()

            @pl.when(core != g % 2)
            def _():
                far.wait_send()


def shards(chips, bands, wave_rows, projectors, dij_table, dij_index, proj_count):
    depth = dij_index.shape[0] * dij_table.shape[1]
    all_rows, columns = wave_rows.shape
    length = chips // 2
    width = columns // 2
    both = 2 * depth
    groups = GROUPS
    rows = 2 * all_rows // groups
    others = max(bands - 1, 1)
    gather_plan = [chunks_of(width, share) for share in GATHER_SHARE]
    scatter_plan = [chunks_of(width, share) for share in SCATTER_SHARE]
    steps = orders_of(length, gather_plan, scatter_plan)
    chunks = max(len(p) for p in gather_plan + scatter_plan)
    flows = max(len(flows_of(p)) for p in gather_plan + scatter_plan)
    dma = pltpu.SemaphoreType.DMA
    f32, bf16 = jnp.float32, jnp.bfloat16
    anywhere = pl.BlockSpec(memory_space=pl.ANY)
    return pl.pallas_call(
        functools.partial(kernel, length, bands, gather_plan, scatter_plan, steps),
        out_shape=jax.ShapeDtypeStruct((all_rows, columns), bf16),
        in_specs=[anywhere] * 5,
        out_specs=anywhere,
        scratch_shapes=[
            pltpu.VMEM((groups, 2, length, rows, width), bf16),
            pltpu.VMEM((both, width), bf16),
            pltpu.VMEM((groups, 2, length, rows, width), f32),
            pltpu.VMEM((groups, length, rows, width), bf16),
            pltpu.VMEM((groups, length, rows, width), bf16),
            pltpu.VMEM((groups, 2, length + 1, rows, width), bf16),
            pltpu.VMEM((groups, 2, length * rows, both), f32),
            pltpu.VMEM((groups, length * rows, both), f32),
            pltpu.VMEM((groups, others, length * rows, both), f32),
            pltpu.VMEM((2, depth, depth), f32),
            pltpu.VMEM((groups, 2, length * rows, both), bf16),
            pltpu.VMEM(dij_table.shape[1:] + dij_table.shape[:1], f32),
            pltpu.SMEM(dij_index.shape, jnp.int32), pltpu.SMEM(proj_count.shape, jnp.int32),
            dma((3,)), dma((groups // 2 + 1,)), dma((2, groups // 2)), dma((2,)), dma((2,)),
            dma((groups, flows)), dma((groups, flows, length)),
            dma((groups, chunks)), dma((groups, chunks)),
            dma((groups, flows)), dma((groups, flows, length + 1)),
            dma((groups, chunks)), dma((groups, chunks, length)),
            dma((2, groups)), dma((groups, others)), dma((groups, others)), dma((2, groups)),
            dma((2, groups, chunks)), dma((groups, chunks)),
        ],
        compiler_params=pltpu.CompilerParams(
            collective_id=0, has_side_effects=True, vmem_limit_bytes=60 * 1024 * 1024
        ),
    )(wave_rows, projectors, jnp.transpose(dij_table, (1, 2, 0)), dij_index, proj_count)


def solution(mesh):
    in_specs = (P("atom", "band"), P("atom", "band"), P(), P("atom"), P("atom"))
    chips = mesh.shape["atom"] // 2
    bands = mesh.shape["band"]
    return jax.jit(
        jax.shard_map(
            functools.partial(shards, chips, bands),
            mesh=mesh,
            in_specs=in_specs,
            out_specs=P("atom", "band"),
            check_vma=False,
        )
    )
```
